256 devices in a mesh: gx: 8 (over y, core), gy: 32 (over z, x).
Axes of the slice: x: 4, y: 4, z: 8, core: 2. Of those that a mesh axis runs over, the one named last changes fastest.
Arguments:
- pressure: float32 [512, 512, 512], P('gx', 'gy'), may hold values from -6 to 6
- divergence: float32 [512, 512, 512], P('gx', 'gy'), may hold values from -6 to 6
- diagonal: float32 [512, 512, 512], P('gx', 'gy'), may hold values from 0.05 to 0.5
- normals: float32 [3, 262144], P(None, ('gx', 'gy')), may hold values from -6 to 6
- traction: float32 [3, 262144], P(None, ('gx', 'gy')), may hold values from -3 to 3
- slot_of: int32 [8, 32768], P('gx'), may hold values from 0 to 98303, as said below
- counts: int32 [256], P(('gx', 'gy')), may hold values from 0 to 3072, as said below
- previous: float32 [3, 786432], P(None, ('gx', 'gy')), may hold values from -6 to 6
- secant_v: float32 [32, 3, 786432], P(None, None, ('gx', 'gy')), may hold values from -6 to 6
- secant_w: float32 [32, 3, 786432], P(None, None, ('gx', 'gy')), may hold values from -940.60406 to 940.60406
Outputs:
- pressure_new: float32 [512, 512, 512], P('gx', 'gy')
- coupled: float32 [3, 786432], P(None, ('gx', 'gy'))
The draws below stay inside these ranges and needn't reach their ends.
Inputs may be any that keep to these rules, and one draw needn't show every extreme that they name: Within each group (row of slot_of) the places are distinct; place o * 3072 + s has s < counts[a * 32 + o]; every such place is used; the rows of one device (aligned blocks of 1024 entries) send at most 96 rows to one owner, and exactly 96 to some owner. The counts of one group sum to 32768; some owner of every group holds exactly 3072.
All inputs are finite; a program needn't handle non-finite values.
Results may differ from the reference program's by a relative error of at most 0.00019.
Values sent between devices are 32-bit elements; how exact they have to be, the bound alone decides.
A program may use at most 128 MiB of HBM per device.

```python
import math
import jax
import jax.numpy as jnp
from jax import lax

CX = 64
CY = 16
CZ = 512
SWEEPS = 2
K = 32
R_DEV = 1024
G_ROWS = 32768
NROWS = 262144
PAIR = 96
HEAVY = 4
CAP = 3072
OWN = 786432
NX = 512
NY = 512
N_GX = 8
N_GY = 32


def plan_group(group_key):
    first_key, second_key, third_key = jax.random.split(group_key, 3)
    owner_order = jax.random.permutation(first_key, N_GY)

    def one_source(source_key):
        position = jax.random.permutation(source_key, R_DEV)
        heavy_index = position // PAIR
        light_index = HEAVY + (position - HEAVY * PAIR) % (N_GY - HEAVY)
        chosen = jnp.where(position < HEAVY * PAIR, heavy_index, light_index)
        return owner_order[chosen]
    owners = jax.vmap(one_source)(jax.random.split(second_key, N_GY)).reshape(G_ROWS).astype(jnp.int32)
    tiebreak = jax.random.permutation(third_key, G_ROWS).astype(jnp.int32)
    score = owners * G_ROWS + tiebreak
    order = jnp.argsort(score, stable=True)
    owner_counts = jnp.sum((owners[:, None] == jnp.arange(N_GY, dtype=jnp.int32)[None, :]).astype(jnp.int32), axis=0)
    starts = jnp.cumsum(owner_counts) - owner_counts
    sorted_owner = owners[order]
    ranks = jnp.arange(G_ROWS, dtype=jnp.int32) - starts[sorted_owner]
    slots = jnp.zeros((G_ROWS,), jnp.int32).at[order].set(sorted_owner * CAP + ranks)
    return (slots, owner_counts)


def plan_all(key):
    base = jax.random.fold_in(key, 4711)
    group_keys = jax.vmap(lambda index: jax.random.fold_in(base, index))(jnp.arange(N_GX))
    return jax.vmap(plan_group)(group_keys)


def draw_slot_of(key, part):
    slots, owner_counts = plan_all(key)
    return slots


def draw_counts(key, part):
    slots, owner_counts = plan_all(key)
    return owner_counts.reshape(N_GX * N_GY)


def shard_levels(key, shape, cuts, low, high):
    gain, own = 1.0, jax.random.fold_in(key, 6)
    for dim, parts in cuts:
        heights = jnp.exp(jax.random.uniform(jax.random.fold_in(own, dim), (parts,), jnp.float32, low / len(cuts), high / len(cuts)))
        gain = gain * jnp.repeat(heights, shape[dim] // parts).reshape([-1 if axis == dim else 1 for axis in range(len(shape))])
    return gain


def noise(rng, shape, scale, reach, pieces=(), held_as=jnp.bfloat16):
    drawn = jax.random.normal(rng, shape, jnp.float32) * scale
    if len(pieces) > 0:
        drawn = shard_levels(rng, shape, pieces, -0.22, 0.18) * drawn
    return jnp.clip(drawn, min=-reach, max=reach).astype(held_as)


def setup_inputs(seed: int = 0) -> dict:
    streams_of = jax.random.split(jax.random.key(seed), 11)
    return {
        "pressure": noise(streams_of[0], (NX, NY, CZ), 1.0, 6.0, ((0, 8), (1, 32)), jnp.float32),
        "divergence": noise(streams_of[1], (NX, NY, CZ), 1.0, 6.0, ((0, 8), (1, 32)), jnp.float32),
        "diagonal": jnp.clip(jnp.exp(math.log(0.5) - 2.3025851 * jax.random.uniform(streams_of[2], (NX, NY, CZ), jnp.float32) ** shard_levels(streams_of[2], (NX, NY, CZ), ((0, 8), (1, 32)), -0.2, 0.2)), 0.05, 0.5),
        "normals": noise(streams_of[3], (3, NROWS), 1.0, 6.0, ((1, 256),), jnp.float32),
        "traction": noise(streams_of[4], (3, NROWS), 0.5, 3.0, ((1, 256),), jnp.float32),
        "slot_of": draw_slot_of(jax.random.fold_in(streams_of[10], 71), 0),
        "counts": draw_counts(jax.random.fold_in(streams_of[10], 71), 0),
        "previous": noise(streams_of[7], (3, OWN), 1.0, 6.0, ((1, 256),), jnp.float32),
        "secant_v": noise(streams_of[8], (K, 3, OWN), 1.0, 6.0, ((2, 256),), jnp.float32),
        "secant_w": noise(streams_of[9], (K, 3, OWN), ((3 * NROWS / K) ** 0.5), 940.60406, ((2, 256),), jnp.float32),
    }


def neighbours(field):
    padded = jnp.pad(field, 1)
    total = padded[2:, 1:-1, 1:-1] + padded[:-2, 1:-1, 1:-1]
    total = total + padded[1:-1, 2:, 1:-1] + padded[1:-1, :-2, 1:-1]
    total = total + padded[1:-1, 1:-1, 2:] + padded[1:-1, 1:-1, :-2]
    return total

def place_group(group_rows, group_slots):
    empty = jnp.zeros((3, N_GY * CAP), jnp.float32)
    return empty.at[:, group_slots].set(group_rows)

def reference(pressure, divergence, diagonal, normals, traction, slot_of, counts, previous, secant_v, secant_w):
    field = pressure
    for sweep_index in range(SWEEPS):
        field = (divergence + neighbours(field)) / (6.0 + diagonal)
    surface = field[:, :, CZ - 1].reshape(N_GX, CX, N_GY, CY).transpose(0, 2, 1, 3).reshape(NROWS)
    forces = normals * surface[None, :] + traction
    grouped = forces.reshape(3, N_GX, G_ROWS).transpose(1, 0, 2)
    owned = jax.vmap(place_group)(grouped, slot_of)
    owned = owned.reshape(N_GX, 3, N_GY * CAP).transpose(1, 0, 2).reshape(3, OWN)
    slot_index = jnp.arange(CAP, dtype=jnp.int32)
    occupied = (slot_index[None, :] < counts[:, None]).astype(jnp.float32).reshape(OWN)
    residual = occupied[None, :] * (owned - previous)
    masked_v = (secant_v * occupied[None, None, :]).reshape(K, 3 * OWN)
    gram = jnp.dot(masked_v, masked_v.T, precision=lax.Precision.HIGHEST)
    projection = jnp.dot(masked_v, residual.reshape(3 * OWN), precision=lax.Precision.HIGHEST)
    factor = jnp.linalg.cholesky(gram)
    coefficient = -jax.scipy.linalg.cho_solve((factor, True), projection)
    update = jnp.dot(coefficient, secant_w.reshape(K, 3 * OWN), precision=lax.Precision.HIGHEST).reshape(3, OWN)
    coupled = occupied[None, :] * (owned + update)
    return (field, coupled)
```

```python
import functools

import jax
import jax.numpy as jnp
from jax import lax
from jax.experimental import pallas as pl
from jax.experimental.pallas import tpu as pltpu
from jax.sharding import PartitionSpec as P

MESH = pl.DeviceIdType.MESH
F32 = jnp.float32
BF16 = jnp.bfloat16
NT = (((1,), (1,)), ((), ()))


def nt_dot(a, b):
    return lax.dot_general(a, b, NT, preferred_element_type=F32)


def split3(x):
    hi = x.astype(BF16).astype(F32)
    rest = x - hi
    mid = rest.astype(BF16).astype(F32)
    return hi, mid, rest - mid


def kernel(
    ngx, ngy,
    p_hbm, d_hbm, g_hbm, n_hbm, t_hbm, slot_hbm, cnt_hbm, prev_hbm, v_hbm, w_hbm,
    out_p, out_c,
    pp, pq, dv, gd, ob, vv, ww, nrm, trc, slt, cnt, prv, outc,
    slab, num, ons, bt1, mh, bt2, amat, xs,
    fj, fi, fc, ssb, srb, fsb, frb, gsb, grb, hsb, hrb, psb, prb, qsb, qrb,
    in_sem, out_sem, fs_sem, fr_sem, hs_sem, hr_sem, as_sem, ar_sem,
):
    gx = lax.axis_index("gx")
    gy = lax.axis_index("gy")
    K = 32
    CAPR = 24

    def wrap(i, n):
        return lax.rem(i + n, n)

    bar = pltpu.get_barrier_semaphore()
    for d in range(1, ngy):
        pl.semaphore_signal(bar, inc=1, device_id=(gx, wrap(gy + d, ngy)), device_id_type=MESH)
    for d in range(1, ngx):
        pl.semaphore_signal(bar, inc=1, device_id=(wrap(gx + d, ngx), gy), device_id_type=MESH)
    for a in (-1, 1):
        for b in (-1, 1):
            pl.semaphore_signal(
                bar, inc=1, device_id=(wrap(gx + a, ngx), wrap(gy + b, ngy)), device_id_type=MESH
            )

    copies = []

    def load(src, dst):
        c = pltpu.make_async_copy(src, dst, in_sem.at[len(copies)])
        c.start()
        copies.append(c)
        return c

    c_slot = load(slot_hbm.at[:, pl.ds(pl.multiple_of(gy * 1024, 1024), 1024)], slt)
    c_cnt = load(cnt_hbm, cnt)

    def tile_loads(t):
        lanes = pl.ds(128 * t, 128)
        return (
            load(p_hbm.at[:, :, lanes], pp.at[t, pl.ds(1, 64), pl.ds(8, 16), :]),
            load(d_hbm.at[:, :, lanes], dv.at[t]),
            load(g_hbm.at[:, :, lanes], gd.at[t]),
        )

    c_t3 = tile_loads(3)
    c_v = load(v_hbm, vv)
    c_n = load(n_hbm, nrm)
    c_t = load(t_hbm, trc)
    c_prev = load(prev_hbm, prv)
    c_rest = [c for t in range(3) for c in tile_loads(t)]
    c_w = load(w_hbm, ww)

    has_im, has_ip = gx > 0, gx < ngx - 1
    has_jm, has_jp = gy > 0, gy < ngy - 1

    def both(a, b):
        return jnp.logical_and(a, b)

    def zero_when(cond, ref):
        @pl.when(jnp.logical_not(cond))
        def _():
            ref[...] = jnp.zeros(ref.shape, ref.dtype)

    for f in (pp, pq):
        zero_when(has_im, f.at[:, 0:1, 8:24, :])
        zero_when(has_ip, f.at[:, 65:66, 8:24, :])
        zero_when(has_jm, f.at[:, 1:65, 7:8, :])
        zero_when(has_jp, f.at[:, 1:65, 24:25, :])
    zero_when(has_jm, fj.at[0])
    zero_when(has_jp, fj.at[1])
    zero_when(has_im, fi.at[0])
    zero_when(has_ip, fi.at[1])
    corner_has = (both(has_im, has_jm), both(has_im, has_jp), both(has_ip, has_jm), both(has_ip, has_jp))
    for k in range(4):
        zero_when(corner_has[k], fc.at[k])

    c_slot.wait()
    slot = slt[...].astype(F32)
    owner = jnp.floor((slot + 0.5) * (1.0 / 3072.0))
    place = slot - owner * 3072.0
    place_hi = jnp.floor((place + 0.5) * (1.0 / 256.0))
    place_lo = place - place_hi * 256.0
    oidx = lax.broadcasted_iota(jnp.int32, (32, 1024), 0).astype(F32)
    onehot = (oidx == owner).astype(F32)
    ons[...] = onehot
    upper = (
        lax.broadcasted_iota(jnp.int32, (128, 128), 0) > lax.broadcasted_iota(jnp.int32, (128, 128), 1)
    ).astype(BF16)
    ones = jnp.ones((128, 128), BF16)
    parts = [onehot[:, 128 * t : 128 * t + 128] for t in range(8)]
    stack = jnp.concatenate(parts, axis=0).astype(BF16)
    before = nt_dot(stack, upper)
    total = nt_dot(stack, ones)
    carry = jnp.zeros((32, 128), F32)
    ridx = lax.broadcasted_iota(jnp.int32, (128, 128), 0).astype(F32)
    for t in range(8):
        rank = jnp.sum(parts[t] * (before[32 * t : 32 * t + 32] + carry), axis=0, keepdims=True)
        carry = carry + total[32 * t : 32 * t + 32]
        bt1[:, 128 * t : 128 * t + 128] = (ridx == rank).astype(BF16)
    a2 = jnp.concatenate([onehot * place_hi, onehot * place_lo], axis=0).astype(BF16)
    sent = nt_dot(a2, bt1[...])
    ssb[0] = sent[:32]
    ssb[1] = sent[32:]
    srb[:, pl.ds(gy, 1), :] = ssb[:, pl.ds(gy, 1), :]

    for c in c_t3:
        c.wait()
    for t in range(8):
        lanes = slice(128 * t, 128 * t + 128)
        for k, x in enumerate(
            (
                pp[3, 1 + 8 * t : 9 + 8 * t, 8:24, :],
                dv[3, 8 * t : 8 * t + 8],
                gd[3, 8 * t : 8 * t + 8],
            )
        ):
            num[k, :, lanes] = x.reshape(128, 128).T[120:128]
    lane = lax.broadcasted_iota(jnp.int32, (8, 1024), 1)
    row = lax.broadcasted_iota(jnp.int32, (8, 1024), 0)
    jj = lane & 15
    P8 = num[0]
    D8 = num[1]
    R8 = 1.0 / (6.0 + num[2])

    def lateral(x):
        s = jnp.where(jj > 0, pltpu.roll(x, 1, 1), 0.0) + jnp.where(jj < 15, pltpu.roll(x, 1023, 1), 0.0)
        return s + jnp.where(lane >= 16, pltpu.roll(x, 16, 1), 0.0) + jnp.where(lane < 1008, pltpu.roll(x, 1008, 1), 0.0)

    N8 = D8 + pltpu.roll(P8, 1, 0) + jnp.where(row < 7, pltpu.roll(P8, 7, 0), 0.0) + lateral(P8)
    num[2] = R8
    num[3] = N8
    slab[...] = jnp.where(
        row >= 6, P8, jnp.where(row == 5, pltpu.roll(N8, 6, 0), pltpu.roll(R8, 5, 0))
    )

    c_cnt.wait()
    c_v.wait()
    count = cnt[0]
    gram = jnp.zeros((96, 128), F32)
    for c in range(3):
        for q in range(6):
            lo = 512 * q
            keep = lax.broadcasted_iota(jnp.int32, (K, 512), 1) + lo < count
            x = jnp.where(keep, vv[c, :, lo : lo + 512], 0.0)
            hi, mid, low = split3(x)
            s = jnp.concatenate([hi, mid, low, jnp.zeros_like(hi)], axis=0).astype(BF16)
            gram = gram + nt_dot(s[:96], s)
    gram = gram[0:32] + gram[32:64] + gram[64:96]
    gram = gram + pltpu.roll(gram, 96, 1) + pltpu.roll(gram, 64, 1)
    lane32 = lax.broadcasted_iota(jnp.int32, (32, 128), 1)
    gram = jnp.where(lane32 < 32, gram, 0.0)
    packed = gram[0:8]
    for t in range(1, 4):
        packed = packed + pltpu.roll(gram[8 * t : 8 * t + 8], 32 * t, 1)
    gsb[...] = packed
    grb[pl.ds(gy, 1)] = packed[None]

    pl.semaphore_wait(bar, (ngy - 1) + (ngx - 1) + 4)

    def remote(src, dst, ss, rs, dev):
        return pltpu.make_async_remote_copy(
            src_ref=src, dst_ref=dst, send_sem=ss, recv_sem=rs, device_id=dev, device_id_type=MESH
        )

    jm, jp = (gx, gy - 1), (gx, gy + 1)
    im, ip = (gx - 1, gy), (gx + 1, gy)
    lo_t, hi_t = pl.ds(0, 128), pl.ds(896, 128)
    faces = [
        (has_jm, jm, slab, fj.at[1], 1, 0),
        (has_jp, jp, slab, fj.at[0], 0, 1),
        (has_im, im, slab.at[:, lo_t], fi.at[1], 3, 2),
        (has_ip, ip, slab.at[:, hi_t], fi.at[0], 2, 3),
        (corner_has[0], (gx - 1, gy - 1), slab.at[:, lo_t], fc.at[3], 7, 4),
        (corner_has[1], (gx - 1, gy + 1), slab.at[:, lo_t], fc.at[2], 6, 5),
        (corner_has[2], (gx + 1, gy - 1), slab.at[:, hi_t], fc.at[1], 5, 6),
        (corner_has[3], (gx + 1, gy + 1), slab.at[:, hi_t], fc.at[0], 4, 7),
    ]
    face_dst = [fj.at[0], fj.at[1], fi.at[0], fi.at[1], fc.at[0], fc.at[1], fc.at[2], fc.at[3]]
    for cond, dev, src, dst, there, here in faces:
        @pl.when(cond)
        def _(dev=dev, src=src, dst=dst, there=there, here=here):
            remote(src, dst, fs_sem.at[here], fr_sem.at[there], dev).start()

    def to_group(src_of, dst, ss, rs):
        for d in range(1, ngy):
            o = wrap(gy + d, ngy)
            remote(src_of(o), dst, ss, rs, (gx, o)).start()

    def to_line(src, dst, ss, rs):
        for d in range(1, ngx):
            remote(src, dst, ss, rs, (wrap(gx + d, ngx), gy)).start()

    def wait_bytes(ref, sem):
        pltpu.make_async_copy(ref, ref, sem).wait()

    to_group(lambda o: ssb.at[:, pl.ds(o, 1), :], srb.at[:, pl.ds(gy, 1), :], as_sem.at[0], ar_sem.at[0])

    def halos(f, base):
        return [
            (has_jm, jm, f.at[:, 1:65, 8:9, :], f.at[:, 1:65, 24:25, :], base + 1, base + 0),
            (has_jp, jp, f.at[:, 1:65, 23:24, :], f.at[:, 1:65, 7:8, :], base + 0, base + 1),
            (has_im, im, f.at[:, 1:2, 8:24, :], f.at[:, 65:66, 8:24, :], base + 3, base + 2),
            (has_ip, ip, f.at[:, 64:65, 8:24, :], f.at[:, 0:1, 8:24, :], base + 2, base + 3),
        ]

    def send_halos(f, base):
        for cond, dev, src, dst, there, here in halos(f, base):
            @pl.when(cond)
            def _(dev=dev, src=src, dst=dst, there=there, here=here):
                remote(src, dst, hs_sem.at[here], hr_sem.at[there], dev).start()

    def wait_halos(f, base):
        into = (f.at[:, 1:65, 7:8, :], f.at[:, 1:65, 24:25, :], f.at[:, 0:1, 8:24, :], f.at[:, 65:66, 8:24, :])
        for (cond, dev, src, dst, there, here), mine in zip(halos(f, base), into):
            @pl.when(cond)
            def _(dev=dev, src=src, mine=mine, here=here):
                remote(src, mine, hs_sem.at[here], hr_sem.at[here], dev).wait_recv()

    def wait_halos_sent(f, base):
        for cond, dev, src, dst, there, here in halos(f, base):
            @pl.when(cond)
            def _(dev=dev, src=src, dst=dst, there=there, here=here):
                remote(src, dst, hs_sem.at[here], hr_sem.at[here], dev).wait_send()

    for c in c_rest:
        c.wait()
    send_halos(pp, 0)
    to_group(lambda o: gsb, grb.at[gy], as_sem.at[1], ar_sem.at[1])

    for (cond, dev, src, dst, there, here), mine in zip(faces, face_dst):
        @pl.when(cond)
        def _(dev=dev, src=src, mine=mine, here=here):
            remote(src, mine, fs_sem.at[here], fr_sem.at[here], dev).wait_recv()
    a_jm = jnp.where(jj == 0, pltpu.roll(fj[0], 1009, 1), 0.0)
    a_jp = jnp.where(jj == 15, pltpu.roll(fj[1], 15, 1), 0.0)
    lane1 = lax.broadcasted_iota(jnp.int32, (8, 128), 1)
    gap = jnp.zeros((8, 768), F32)
    a_i = jnp.concatenate(
        [
            jnp.where(lane1 < 16, pltpu.roll(fi[0], 16, 1), 0.0),
            gap,
            jnp.where(lane1 >= 112, pltpu.roll(fi[1], 112, 1), 0.0),
        ],
        axis=1,
    )
    corner = jnp.concatenate(
        [
            jnp.where(lane1 == 0, pltpu.roll(fc[0], 1, 1), 0.0)
            + jnp.where(lane1 == 15, pltpu.roll(fc[1], 31, 1), 0.0),
            gap,
            jnp.where(lane1 == 112, pltpu.roll(fc[2], 97, 1), 0.0)
            + jnp.where(lane1 == 127, pltpu.roll(fc[3], 127, 1), 0.0),
        ],
        axis=1,
    )
    P8 = num[0]
    D8 = num[1]
    R8 = num[2]
    once = (num[3] + a_jm + a_jp + a_i) * R8
    base = P8[7:8] + corner[7:8]
    beyond = (
        (a_jm[5:6] + base) * a_jm[4:5] + (a_jp[5:6] + base) * a_jp[4:5] + (a_i[5:6] + base) * a_i[4:5]
    )
    surface = (D8[7:8] + once[6:7] + lateral(once)[7:8] + beyond) * R8[7:8]
    c_n.wait()
    c_t.wait()
    forces = nrm[...] * surface + trc[...]

    onehot = ons[...]
    rows = []
    for piece in split3(forces):
        for c in range(3):
            rows.append((onehot * piece[c : c + 1]).astype(BF16))
    moved = nt_dot(jnp.concatenate(rows, axis=0), bt1[...])
    moved = moved[0:96] + moved[96:192] + moved[192:288]
    for c in range(3):
        fsb[c] = moved[32 * c : 32 * c + 32]
    frb[:, pl.ds(gy, 1), :] = fsb[:, pl.ds(gy, 1), :]
    to_group(lambda o: fsb.at[:, pl.ds(o, 1), :], frb.at[:, pl.ds(gy, 1), :], as_sem.at[2], ar_sem.at[2])

    lane2 = lax.broadcasted_iota(jnp.int32, (16, 128), 1)

    def plane_sum(f, i):
        xs_ = [f[t, i + 1, 8:24, :] for t in range(4)]
        rr = [pltpu.roll(x, 1, 1) for x in xs_]
        rl = [pltpu.roll(x, 127, 1) for x in xs_]
        zero = jnp.zeros((16, 128), F32)
        res = []
        for t in range(4):
            down = jnp.where(lane2 == 0, rr[t - 1] if t > 0 else zero, rr[t])
            up = jnp.where(lane2 == 127, rl[t + 1] if t < 3 else zero, rl[t])
            s = f[t, i, 8:24, :] + f[t, i + 2, 8:24, :]
            s = s + (f[t, i + 1, 7:23, :] + f[t, i + 1, 9:25, :])
            res.append(dv[t, i] + s + (up + down))
        return res

    wait_halos(pp, 0)

    def sweep1(i, carry):
        sums = plane_sum(pp, i)
        for t in range(4):
            r = 1.0 / (6.0 + gd[t, i])
            gd[t, i] = r
            pq[t, i + 1, 8:24, :] = sums[t] * r
        return carry

    lax.fori_loop(0, 64, sweep1, 0, unroll=2)
    send_halos(pq, 4)

    wait_bytes(srb.at[:, pl.ds(0, ngy - 1), :], ar_sem.at[0])
    hidx = lax.broadcasted_iota(jnp.int32, (16, 128), 0).astype(F32)
    lidx = lax.broadcasted_iota(jnp.int32, (256, 128), 0).astype(F32)
    for b in range(ngy):
        lanes = slice(128 * b, 128 * b + 128)
        mh[:, lanes] = (hidx == srb[0, b : b + 1, :]).astype(F32)
        bt2[:, lanes] = (lidx == srb[1, b : b + 1, :]).astype(BF16)

    wait_bytes(grb.at[pl.ds(0, ngy - 1)], ar_sem.at[1])
    packed = jnp.sum(grb[...], axis=0)
    hsb[...] = packed
    hrb[pl.ds(gx, 1)] = packed[None]
    to_line(hsb, hrb.at[gx], as_sem.at[3], ar_sem.at[3])

    wait_bytes(frb.at[:, pl.ds(0, ngy - 1), :], ar_sem.at[2])
    for c in range(3):
        pieces = split3(frb[c])
        for b in range(ngy):
            lanes = slice(128 * b, 128 * b + 128)
            m = mh[:, lanes]
            for s in range(3):
                r0 = 48 * s + 16 * c
                amat[r0 : r0 + 16, lanes] = (m * pieces[s][b : b + 1]).astype(BF16)
    own = nt_dot(amat[...], bt2[...])
    xs[...] = own[0:48] + own[48:96] + own[96:144]
    c_prev.wait()

    def slot_row(ref, c, h):
        return ref[16 * c + h // 2 : 16 * c + h // 2 + 1, 128 * (h % 2) : 128 * (h % 2) + 128]

    lane_row = lax.broadcasted_iota(jnp.int32, (1, 128), 1)
    acc = [jnp.zeros((8, 128), F32) for _ in range(4)]
    for h in range(CAPR):
        keep = lane_row + 128 * h < count
        lanes = slice(128 * h, 128 * h + 128)
        for c in range(3):
            res = jnp.where(keep, slot_row(xs, c, h) - prv[c : c + 1, lanes], 0.0)
            for k in range(4):
                acc[k] = acc[k] + vv[c, 8 * k : 8 * k + 8, lanes] * res
    diag = lax.broadcasted_iota(jnp.int32, (32, 128), 0) == lane32

    def to_row(col):
        return jnp.sum(jnp.where(diag, col, 0.0), axis=0, keepdims=True)

    def to_col(r):
        return jnp.sum(jnp.where(diag, r, 0.0), axis=1, keepdims=True)

    prow = to_row(jnp.sum(jnp.concatenate(acc, axis=0), axis=1, keepdims=True))
    psb[...] = prow
    prb[pl.ds(gy, 1), :] = prow
    to_group(lambda o: psb, prb.at[pl.ds(gy, 1), :], as_sem.at[4], ar_sem.at[4])

    wait_halos(pq, 4)

    def sweep2(i, carry):
        sums = plane_sum(pq, i)
        for t in range(4):
            ob[t, i] = sums[t] * gd[t, i]
        return carry

    c_out = []
    for q in range(4):
        lax.fori_loop(16 * q, 16 * q + 16, sweep2, 0, unroll=2)
        for t in range(4):
            c = pltpu.make_async_copy(
                ob.at[t, pl.ds(16 * q, 16)],
                out_p.at[pl.ds(16 * q, 16), :, pl.ds(128 * t, 128)],
                out_sem.at[4 * q + t],
            )
            c.start()
            c_out.append(c)

    wait_bytes(hrb.at[pl.ds(0, ngx - 1)], ar_sem.at[3])
    packed = jnp.sum(hrb[...], axis=0)
    m = jnp.concatenate([packed] + [pltpu.roll(packed, 128 - 32 * t, 1) for t in range(1, 4)], axis=0)
    sub32 = lax.broadcasted_iota(jnp.int32, (32, 128), 0)
    m = jnp.where(lane32 < 32, m, (sub32 + 32 == lane32).astype(F32))
    dinv = jnp.zeros((32, 1), F32)
    sub1 = lax.broadcasted_iota(jnp.int32, (32, 1), 0)
    for k in range(K):
        r = m[k : k + 1]
        inv = 1.0 / r[:, k : k + 1]
        dinv = jnp.where(sub1 == k, inv, dinv)
        if k < K - 1:
            f = jnp.where(sub1 > k, m[:, k : k + 1] * inv, 0.0)
            m = m - f * r
    linv = jnp.where(lane32 < 32, pltpu.roll(m, 96, 1), 0.0)

    wait_bytes(prb.at[pl.ds(0, ngy - 1), :], ar_sem.at[4])
    prow = jnp.sum(prb[...], axis=0, keepdims=True)
    qsb[...] = prow
    qrb[pl.ds(gx, 1), :] = prow
    to_line(qsb, qrb.at[pl.ds(gx, 1), :], as_sem.at[5], ar_sem.at[5])
    c_w.wait()
    wait_bytes(qrb.at[pl.ds(0, ngx - 1), :], ar_sem.at[5])
    prow = jnp.sum(qrb[...], axis=0, keepdims=True)
    y = jnp.sum(linv * prow, axis=1, keepdims=True) * dinv
    coef = to_col(-jnp.sum(linv * y, axis=0, keepdims=True))
    cb = [jnp.broadcast_to(coef[8 * k : 8 * k + 8], (8, 128)) for k in range(4)]
    for h in range(CAPR):
        keep = lane_row + 128 * h < count
        lanes = slice(128 * h, 128 * h + 128)
        for c in range(3):
            u = cb[0] * ww[c, 0:8, lanes] + cb[1] * ww[c, 8:16, lanes]
            u = u + (cb[2] * ww[c, 16:24, lanes] + cb[3] * ww[c, 24:32, lanes])
            u = jnp.sum(u, axis=0, keepdims=True)
            outc[c : c + 1, lanes] = jnp.where(keep, slot_row(xs, c, h) + u, 0.0)
    c = pltpu.make_async_copy(outc, out_c, out_sem.at[16])
    c.start()
    c_out.append(c)

    for cond, dev, src, dst, there, here in faces:
        @pl.when(cond)
        def _(dev=dev, src=src, dst=dst, here=here):
            remote(src, dst, fs_sem.at[here], fr_sem.at[here], dev).wait_send()
    wait_halos_sent(pp, 0)
    wait_halos_sent(pq, 4)
    wait_bytes(srb.at[:, pl.ds(0, ngy - 1), :], as_sem.at[0])
    wait_bytes(grb.at[pl.ds(0, ngy - 1)], as_sem.at[1])
    wait_bytes(frb.at[:, pl.ds(0, ngy - 1), :], as_sem.at[2])
    wait_bytes(hrb.at[pl.ds(0, ngx - 1)], as_sem.at[3])
    wait_bytes(prb.at[pl.ds(0, ngy - 1), :], as_sem.at[4])
    wait_bytes(qrb.at[pl.ds(0, ngx - 1), :], as_sem.at[5])
    for c in c_out:
        c.wait()


def shards(
    ngx, ngy,
    pressure, divergence, diagonal, normals, traction, slot_of, counts, previous, secant_v, secant_w,
):
    v = jnp.transpose(secant_v, (1, 0, 2))
    w = jnp.transpose(secant_w, (1, 0, 2))
    any_spec = pl.BlockSpec(memory_space=pl.ANY)
    vm = pltpu.VMEM
    dma = pltpu.SemaphoreType.DMA
    return pl.pallas_call(
        functools.partial(kernel, ngx, ngy),
        out_shape=(
            jax.ShapeDtypeStruct(pressure.shape, F32),
            jax.ShapeDtypeStruct(previous.shape, F32),
        ),
        in_specs=[any_spec] * 10,
        out_specs=(any_spec, any_spec),
        scratch_shapes=[
            vm((4, 66, 32, 128), F32),
            vm((4, 66, 32, 128), F32),
            vm((4, 64, 16, 128), F32),
            vm((4, 64, 16, 128), F32),
            vm((4, 64, 16, 128), F32),
            vm((3, 32, 3072), F32),
            vm((3, 32, 3072), F32),
            vm((3, 1024), F32),
            vm((3, 1024), F32),
            vm((1, 1024), jnp.int32),
            pltpu.SMEM((1,), jnp.int32),
            vm((3, 3072), F32),
            vm((3, 3072), F32),
            vm((8, 1024), F32),
            vm((4, 8, 1024), F32),
            vm((32, 1024), F32),
            vm((128, 1024), BF16),
            vm((16, 128 * ngy), F32),
            vm((256, 128 * ngy), BF16),
            vm((144, 128 * ngy), BF16),
            vm((48, 256), F32),
            vm((2, 8, 1024), F32),
            vm((2, 8, 128), F32),
            vm((4, 8, 128), F32),
            vm((2, 32, 128), F32),
            vm((2, 32, 128), F32),
            vm((3, 32, 128), F32),
            vm((3, 32, 128), F32),
            vm((8, 128), F32),
            vm((ngy, 8, 128), F32),
            vm((8, 128), F32),
            vm((ngx, 8, 128), F32),
            vm((1, 128), F32),
            vm((ngy, 128), F32),
            vm((1, 128), F32),
            vm((ngx, 128), F32),
            dma((24,)),
            dma((17,)),
            dma((8,)),
            dma((8,)),
            dma((8,)),
            dma((8,)),
            dma((6,)),
            dma((6,)),
        ],
        compiler_params=pltpu.CompilerParams(
            collective_id=0, has_side_effects=True, vmem_limit_bytes=48 * 1024 * 1024
        ),
    )(pressure, divergence, diagonal, normals, traction, slot_of, counts, previous, v, w)


def solution(mesh):
    placed = (
        P("gx", "gy", None),
        P("gx", "gy", None),
        P("gx", "gy", None),
        P(None, ("gx", "gy")),
        P(None, ("gx", "gy")),
        P("gx", None),
        P(("gx", "gy")),
        P(None, ("gx", "gy")),
        P(None, None, ("gx", "gy")),
        P(None, None, ("gx", "gy")),
    )
    return jax.shard_map(
        functools.partial(shards, mesh.shape["gx"], mesh.shape["gy"]),
        mesh=mesh,
        in_specs=placed,
        out_specs=(P("gx", "gy", None), P(None, ("gx", "gy"))),
        check_vma=False,
    )
```

```python
import functools

import jax
import jax.numpy as jnp
from jax import lax
from jax.experimental import pallas as pl
from jax.experimental.pallas import tpu as pltpu
from jax.sharding import PartitionSpec as P

MESH = pl.DeviceIdType.MESH
F32 = jnp.float32
BF16 = jnp.bfloat16
NT = (((1,), (1,)), ((), ()))


def nt_dot(a, b):
    return lax.dot_general(a, b, NT, preferred_element_type=F32)


def split3(x):
    hi = x.astype(BF16).astype(F32)
    rest = x - hi
    mid = rest.astype(BF16).astype(F32)
    return hi, mid, rest - mid


def kernel(
    ngx, ngy,
    p_hbm, d_hbm, g_hbm, n_hbm, t_hbm, slot_hbm, cnt, prev_hbm, v_hbm, w_hbm,
    out_p, ww, xs, occ, cof,
    pp, pq, dv, gd, rv, vv, nrm, trc, slt, prv,
    slab, num, ons, bt1, mh, bt2, amat,
    fj, fi, fc, ssb, srb, fsb, frb, near, msk, acc0, gsb, gxb, gxs, grb, hsb, hrb, psb, prb, qsb, qrb,
    in_sem, fs_sem, fr_sem, hs_sem, hr_sem, as_sem, ar_sem, gr_sem, sl_sem, news,
):
    gx = lax.axis_index("gx")
    gy = lax.axis_index("gy")
    K = 32
    UNROLL = 4
    CAPR = 24

    NZ, NX = ngy // 4, 4
    OFF = sorted(
        ((dz, dx) for dz in range(NZ) for dx in range(NX)),
        key=lambda o: (min(o[0], NZ - o[0]) + min(o[1], NX - o[1]), o),
    )
    gz, gq = lax.div(gy, NX), lax.rem(gy, NX)

    def peer(off):
        return lax.rem(gz + off[0], NZ) * NX + lax.rem(gq + off[1], NX)

    def wrap(i, n):
        return lax.rem(i + n, n)

    copies = []

    def load(src, dst):
        c = pltpu.make_async_copy(src, dst, in_sem.at[len(copies)])
        c.start()
        copies.append(c)
        return c

    def lanes_of(t):
        return pl.ds(128 * t, 128)

    def load_p(t):
        return load(p_hbm.at[:, :, lanes_of(t)], pp.at[t, pl.ds(1, 64), pl.ds(8, 16), :])

    c_t3 = (
        load_p(3),
        load(d_hbm.at[:, :, lanes_of(3)], dv.at[3]),
        load(g_hbm.at[:, :, lanes_of(3)], gd.at[3]),
    )
    bar = pltpu.get_barrier_semaphore()
    greet = [
        (wrap(gx + a, ngx), wrap(gy + b, ngy)) for a in (-1, 0, 1) for b in (-1, 0, 1) if (a, b) != (0, 0)
    ]
    greet += [(gx, peer(o)) for o in ((1, 0), (NZ - 1, 0), (2, 0), (NZ - 2, 0), (0, 1), (0, 3), (0, 2))]
    greet += [(wrap(gx + a, ngx), gy) for a in range(2, ngx - 1)]
    for dev in greet:
        pl.semaphore_signal(bar, inc=1, device_id=dev, device_id_type=MESH)

    c_slot = load(slot_hbm.at[:, pl.ds(pl.multiple_of(gy * 1024, 1024), 1024)], slt)
    c_p = [load_p(t) for t in range(3)]
    c_n = load(n_hbm, nrm)
    c_t = load(t_hbm, trc)
    c_v = load(v_hbm, vv)
    c_dg = [load(d_hbm.at[:, :, lanes_of(t)], dv.at[t]) for t in range(3)]
    c_dg += [load(g_hbm.at[:, :, lanes_of(t)], gd.at[t]) for t in range(3)]
    c_prev = load(prev_hbm, prv)
    c_w = load(w_hbm, ww)

    has_im, has_ip = gx > 0, gx < ngx - 1
    has_jm, has_jp = gy > 0, gy < ngy - 1

    def both(a, b):
        return jnp.logical_and(a, b)

    def zero_when(cond, ref):
        @pl.when(jnp.logical_not(cond))
        def _():
            ref[...] = jnp.zeros(ref.shape, ref.dtype)

    for f in (pp, pq):
        zero_when(has_im, f.at[:, 0:1, 8:24, :])
        zero_when(has_ip, f.at[:, 65:66, 8:24, :])
        zero_when(has_jm, f.at[:, 1:65, 7:8, :])
        zero_when(has_jp, f.at[:, 1:65, 24:25, :])
    zero_when(has_jm, fj.at[0])
    zero_when(has_jp, fj.at[1])
    zero_when(has_im, fi.at[0])
    zero_when(has_ip, fi.at[1])
    corner_has = (both(has_im, has_jm), both(has_im, has_jp), both(has_ip, has_jm), both(has_ip, has_jp))
    for k in range(4):
        zero_when(corner_has[k], fc.at[k])

    def remote(src, dst, ss, rs, dev):
        return pltpu.make_async_remote_copy(
            src_ref=src, dst_ref=dst, send_sem=ss, recv_sem=rs, device_id=dev, device_id_type=MESH
        )

    jm, jp = (gx, gy - 1), (gx, gy + 1)
    im, ip = (gx - 1, gy), (gx + 1, gy)
    lo_t, hi_t = pl.ds(0, 128), pl.ds(896, 128)
    faces = [
        (has_jm, jm, slab.at[4:8], fj.at[1, 4:8], 1, 0),
        (has_jp, jp, slab.at[4:8], fj.at[0, 4:8], 0, 1),
        (has_im, im, slab.at[4:8, lo_t], fi.at[1, 4:8], 3, 2),
        (has_ip, ip, slab.at[4:8, hi_t], fi.at[0, 4:8], 2, 3),
        (corner_has[0], (gx - 1, gy - 1), slab.at[4:8, lo_t], fc.at[3, 4:8], 7, 4),
        (corner_has[1], (gx - 1, gy + 1), slab.at[4:8, lo_t], fc.at[2, 4:8], 6, 5),
        (corner_has[2], (gx + 1, gy - 1), slab.at[4:8, hi_t], fc.at[1, 4:8], 5, 6),
        (corner_has[3], (gx + 1, gy + 1), slab.at[4:8, hi_t], fc.at[0, 4:8], 4, 7),
    ]
    face_dst = [f.at[k, 4:8] for f, n in ((fj, 2), (fi, 2), (fc, 4)) for k in range(n)]
    def to_group(src_of, dst_of, ss, rs_of):
        for r in range(ngy - 1, 0, -1):
            o = peer(OFF[r])
            remote(src_of(o), dst_of(r), ss, rs_of(r), (gx, o)).start()

    def to_line(src, dst, ss, rs):
        for d in range(1, ngx):
            remote(src, dst, ss, rs, (wrap(gx + d, ngx), gy)).start()

    def wait_bytes(ref, sem):
        pltpu.make_async_copy(ref, ref, sem).wait()

    def halos(f, base):
        return [
            (has_jm, jm, f.at[:, 1:65, 8:9, :], f.at[:, 1:65, 24:25, :], base + 1, base + 0),
            (has_jp, jp, f.at[:, 1:65, 23:24, :], f.at[:, 1:65, 7:8, :], base + 0, base + 1),
            (has_im, im, f.at[:, 1:2, 8:24, :], f.at[:, 65:66, 8:24, :], base + 3, base + 2),
            (has_ip, ip, f.at[:, 64:65, 8:24, :], f.at[:, 0:1, 8:24, :], base + 2, base + 3),
        ]

    def send_halos(f, base):
        for cond, dev, src, dst, there, here in halos(f, base):
            @pl.when(cond)
            def _(dev=dev, src=src, dst=dst, there=there, here=here):
                remote(src, dst, hs_sem.at[here], hr_sem.at[there], dev).start()

    def wait_halos(f, base):
        into = (f.at[:, 1:65, 7:8, :], f.at[:, 1:65, 24:25, :], f.at[:, 0:1, 8:24, :], f.at[:, 65:66, 8:24, :])
        for (cond, dev, src, dst, there, here), mine in zip(halos(f, base), into):
            @pl.when(cond)
            def _(dev=dev, src=src, mine=mine, here=here):
                remote(src, mine, hs_sem.at[here], hr_sem.at[here], dev).wait_recv()

    def wait_halos_sent(f, base):
        for cond, dev, src, dst, there, here in halos(f, base):
            @pl.when(cond)
            def _(dev=dev, src=src, dst=dst, there=there, here=here):
                remote(src, dst, hs_sem.at[here], hr_sem.at[here], dev).wait_send()

    for k, c in enumerate(c_t3):
        c.wait()
        for t in range(8):
            x = pp[3, 1 + 8 * t : 9 + 8 * t, 8:24, :] if k == 0 else (dv, gd)[k - 1][3, 8 * t : 8 * t + 8]
            num[k, :, 128 * t : 128 * t + 128] = x.reshape(128, 128).T[120:128]
    lane = lax.broadcasted_iota(jnp.int32, (8, 1024), 1)
    row = lax.broadcasted_iota(jnp.int32, (8, 1024), 0)
    jj = lane & 15
    P8 = num[0]
    D8 = num[1]
    R8 = 1.0 / (6.0 + num[2])

    def lateral(x):
        s = jnp.where(jj > 0, pltpu.roll(x, 1, 1), 0.0) + jnp.where(jj < 15, pltpu.roll(x, 1023, 1), 0.0)
        return s + jnp.where(lane >= 16, pltpu.roll(x, 16, 1), 0.0) + jnp.where(lane < 1008, pltpu.roll(x, 1008, 1), 0.0)

    N8 = D8 + pltpu.roll(P8, 1, 0) + jnp.where(row < 7, pltpu.roll(P8, 7, 0), 0.0) + lateral(P8)
    num[2] = R8
    num[3] = N8
    slab[...] = jnp.where(
        row >= 6, P8, jnp.where(row == 5, pltpu.roll(N8, 6, 0), pltpu.roll(R8, 5, 0))
    )

    pl.semaphore_wait(bar, len(greet))

    for cond, dev, src, dst, there, here in faces:
        @pl.when(cond)
        def _(dev=dev, src=src, dst=dst, there=there, here=here):
            remote(src, dst, fs_sem.at[here], fr_sem.at[there], dev).start()

    for o in ((1, 0), (NZ - 1, 0), (2, 0), (NZ - 2, 0)):
        pl.semaphore_signal(news.at[0], inc=1, device_id=(gx, peer(o)), device_id_type=MESH)

    for c in c_p:
        c.wait()
    send_halos(pp, 0)

    c_slot.wait()
    slot = slt[...].astype(F32)
    owner = jnp.floor((slot + 0.5) * (1.0 / 3072.0))
    place = slot - owner * 3072.0
    place_hi = jnp.floor((place + 0.5) * (1.0 / 256.0))
    place_lo = place - place_hi * 256.0
    oidx = lax.broadcasted_iota(jnp.int32, (32, 1024), 0).astype(F32)
    onehot = (oidx == owner).astype(F32)
    ons[...] = onehot
    upper = (
        lax.broadcasted_iota(jnp.int32, (128, 128), 0) > lax.broadcasted_iota(jnp.int32, (128, 128), 1)
    ).astype(BF16)
    ones = jnp.ones((128, 128), BF16)
    parts = [onehot[:, 128 * t : 128 * t + 128] for t in range(8)]
    stack = jnp.concatenate(parts, axis=0).astype(BF16)
    before = nt_dot(stack, upper)
    total = nt_dot(stack, ones)
    carry = jnp.zeros((32, 128), F32)
    ridx = lax.broadcasted_iota(jnp.int32, (128, 128), 0).astype(F32)
    for t in range(8):
        rank = jnp.sum(parts[t] * (before[32 * t : 32 * t + 32] + carry), axis=0, keepdims=True)
        carry = carry + total[32 * t : 32 * t + 32]
        bt1[:, 128 * t : 128 * t + 128] = (ridx == rank).astype(BF16)
    a2 = jnp.concatenate([onehot * place_hi, onehot * place_lo], axis=0).astype(BF16)
    sent = nt_dot(a2, bt1[...])
    ssb[0] = sent[:32]
    ssb[1] = sent[32:]
    srb[:, 0:1, :] = ssb[:, pl.ds(gy, 1), :]


    c_v.wait()
    count = cnt[0]
    gram = jnp.zeros((96, 128), F32)
    for c in range(3):
        for q in range(6):
            lo = 512 * q
            keep = lax.broadcasted_iota(jnp.int32, (K, 512), 1) + lo < count
            x = jnp.where(keep, vv[c, :, lo : lo + 512], 0.0)
            hi, mid, low = split3(x)
            s = jnp.concatenate([hi, mid, low, jnp.zeros_like(hi)], axis=0).astype(BF16)
            gram = gram + nt_dot(s[:96], s)
    gram = gram[0:32] + gram[32:64] + gram[64:96]
    gram = gram + pltpu.roll(gram, 96, 1) + pltpu.roll(gram, 64, 1)
    lane32 = lax.broadcasted_iota(jnp.int32, (32, 128), 1)
    gram = jnp.where(lane32 < 32, gram, 0.0)
    packed = gram[0:8]
    for t in range(1, 4):
        packed = packed + pltpu.roll(gram[8 * t : 8 * t + 8], 32 * t, 1)
    gsb[...] = packed
    hrb[pl.ds(gx, 1)] = packed[None]
    to_line(gsb, hrb.at[gx], as_sem.at[3], ar_sem.at[3])

    pl.semaphore_wait(news.at[0], 4)
    for o in ((2, 0), (NZ - 2, 0)):
        pl.semaphore_signal(news.at[1], inc=1, device_id=(gx, peer(o)), device_id_type=MESH)

    for c in c_dg:
        c.wait()

    def recip(i, carry):
        for t in range(4):
            rv[t, i] = 1.0 / (6.0 + gd[t, i])
        return carry

    lax.fori_loop(0, 64, recip, 0, unroll=4)

    for (cond, dev, src, dst, there, here), mine in zip(faces, face_dst):
        @pl.when(cond)
        def _(dev=dev, src=src, mine=mine, here=here):
            remote(src, mine, fs_sem.at[here], fr_sem.at[here], dev).wait_recv()
    a_jm = jnp.where(jj == 0, pltpu.roll(fj[0], 1009, 1), 0.0)
    a_jp = jnp.where(jj == 15, pltpu.roll(fj[1], 15, 1), 0.0)
    lane1 = lax.broadcasted_iota(jnp.int32, (8, 128), 1)
    gap = jnp.zeros((8, 768), F32)
    a_i = jnp.concatenate(
        [
            jnp.where(lane1 < 16, pltpu.roll(fi[0], 16, 1), 0.0),
            gap,
            jnp.where(lane1 >= 112, pltpu.roll(fi[1], 112, 1), 0.0),
        ],
        axis=1,
    )
    corner = jnp.concatenate(
        [
            jnp.where(lane1 == 0, pltpu.roll(fc[0], 1, 1), 0.0)
            + jnp.where(lane1 == 15, pltpu.roll(fc[1], 31, 1), 0.0),
            gap,
            jnp.where(lane1 == 112, pltpu.roll(fc[2], 97, 1), 0.0)
            + jnp.where(lane1 == 127, pltpu.roll(fc[3], 127, 1), 0.0),
        ],
        axis=1,
    )
    P8 = num[0]
    D8 = num[1]
    R8 = num[2]
    once = (num[3] + a_jm + a_jp + a_i) * R8
    base = P8[7:8] + corner[7:8]
    beyond = (
        (a_jm[5:6] + base) * a_jm[4:5] + (a_jp[5:6] + base) * a_jp[4:5] + (a_i[5:6] + base) * a_i[4:5]
    )
    surface = (D8[7:8] + once[6:7] + lateral(once)[7:8] + beyond) * R8[7:8]
    c_n.wait()
    c_t.wait()
    forces = nrm[...] * surface + trc[...]

    pl.semaphore_wait(news.at[1], 2)
    to_group(lambda o: ssb.at[:, pl.ds(o, 1), :], lambda r: srb.at[:, r : r + 1, :], as_sem.at[0], lambda r: sl_sem.at[r // 8])

    onehot = ons[...]
    rows = []
    for piece in split3(forces):
        for c in range(3):
            rows.append((onehot * piece[c : c + 1]).astype(BF16))
    moved = nt_dot(jnp.concatenate(rows, axis=0), bt1[...])
    moved = moved[0:96] + moved[96:192] + moved[192:288]
    for c in range(3):
        fsb[c] = moved[32 * c : 32 * c + 32]
    frb[:, 0:1, :] = fsb[:, pl.ds(gy, 1), :]
    to_group(lambda o: fsb.at[:, pl.ds(o, 1), :], lambda r: frb.at[:, r : r + 1, :], as_sem.at[2], lambda r: gr_sem.at[r // 8])

    def slot_row(ref, c, h):
        return ref[16 * c + h // 2 : 16 * c + h // 2 + 1, 128 * (h % 2) : 128 * (h % 2) + 128]

    where = lax.broadcasted_iota(jnp.int32, (48, 256), 0)
    where = (where & 15) * 256 + lax.broadcasted_iota(jnp.int32, (48, 256), 1)
    occ[...] = (where < count).astype(F32)
    c_prev.wait()
    acc = [jnp.zeros((8, 128), F32) for _ in range(4)]
    for h in range(CAPR):
        lanes = slice(128 * h, 128 * h + 128)
        for c in range(3):
            res = slot_row(occ, c, h) * prv[c : c + 1, lanes]
            for k in range(4):
                acc[k] = acc[k] - vv[c, 8 * k : 8 * k + 8, lanes] * res
    for k in range(4):
        acc0[8 * k : 8 * k + 8] = acc[k]

    lane2 = lax.broadcasted_iota(jnp.int32, (16, 128), 1)

    def plane_sum(f, i):
        xs_ = [f[t, i + 1, 8:24, :] for t in range(4)]
        rr = [pltpu.roll(x, 1, 1) for x in xs_]
        rl = [pltpu.roll(x, 127, 1) for x in xs_]
        zero = jnp.zeros((16, 128), F32)
        res = []
        for t in range(4):
            down = jnp.where(lane2 == 0, rr[t - 1] if t > 0 else zero, rr[t])
            up = jnp.where(lane2 == 127, rl[t + 1] if t < 3 else zero, rl[t])
            s = f[t, i, 8:24, :] + f[t, i + 2, 8:24, :]
            s = s + (f[t, i + 1, 7:23, :] + f[t, i + 1, 9:25, :])
            res.append(dv[t, i] + s + (up + down))
        return res

    wait_halos(pp, 0)

    wait_bytes(hrb.at[pl.ds(0, ngx - 1)], ar_sem.at[3])
    packed = jnp.sum(hrb[...], axis=0)
    hsb[...] = packed
    gxb[pl.ds(gq, 1)] = packed[None]
    for d in (2, 1, 3):
        remote(hsb, gxb.at[gq], as_sem.at[1], ar_sem.at[1], (gx, gz * NX + wrap(gq + d, NX))).start()

    def sweep1(i, carry):
        sums = plane_sum(pp, i)
        for t in range(4):
            pq[t, i + 1, 8:24, :] = sums[t] * rv[t, i]
        return carry

    lax.fori_loop(0, 64, sweep1, 0, unroll=UNROLL)


    wait_bytes(gxb.at[pl.ds(0, 3)], ar_sem.at[1])
    packed = jnp.sum(gxb[...], axis=0)
    gxs[...] = packed
    grb[pl.ds(gz, 1)] = packed[None]
    for d in range(NZ - 1, 0, -1):
        e = (d + 1) // 2 if d % 2 else NZ - d // 2
        remote(gxs, grb.at[gz], as_sem.at[6], ar_sem.at[6], (gx, wrap(gz + e, NZ) * NX + gq)).start()

    hidx = lax.broadcasted_iota(jnp.int32, (16, 128), 0).astype(F32)
    lidx = lax.broadcasted_iota(jnp.int32, (256, 128), 0).astype(F32)

    def masks(g):
        first = max(8 * g, 1)
        wait_bytes(srb.at[:, first : 8 * g + 8, :], sl_sem.at[g])
        for b in range(8 * g, 8 * g + 8):
            lanes = slice(128 * b, 128 * b + 128)
            mh[:, lanes] = (hidx == srb[0, b : b + 1, :]).astype(F32)
            bt2[:, lanes] = (lidx == srb[1, b : b + 1, :]).astype(BF16)

    def place(g):
        first = max(8 * g, 1)
        wait_bytes(frb.at[:, first : 8 * g + 8, :], gr_sem.at[g])
        for c in range(3):
            pieces = split3(frb[c, 8 * g : 8 * g + 8, :])
            for b in range(8):
                lanes = slice(1024 * g + 128 * b, 1024 * g + 128 * b + 128)
                m = mh[:, lanes]
                for k in range(3):
                    r0 = 48 * k + 16 * c
                    amat[r0 : r0 + 16, lanes] = (m * pieces[k][b : b + 1]).astype(BF16)
        return nt_dot(amat[:, 1024 * g : 1024 * g + 1024], bt2[:, 1024 * g : 1024 * g + 1024])

    masks(0)
    masks(1)
    near[...] = place(0)
    masks(2)
    near[...] += place(1)
    masks(3)
    near[...] += place(2)

    own = near[...] + place(3)
    own = own[0:48] + own[48:96] + own[96:144]
    xs[...] = own
    msk[...] = own * occ[...]
    acc = [acc0[8 * k : 8 * k + 8] for k in range(4)]
    for h in range(CAPR):
        lanes = slice(128 * h, 128 * h + 128)
        for c in range(3):
            res = slot_row(msk, c, h)
            for k in range(4):
                acc[k] = acc[k] + vv[c, 8 * k : 8 * k + 8, lanes] * res
    diag = lax.broadcasted_iota(jnp.int32, (32, 128), 0) == lane32

    def to_row(col):
        return jnp.sum(jnp.where(diag, col, 0.0), axis=0, keepdims=True)

    def to_col(r):
        return jnp.sum(jnp.where(diag, r, 0.0), axis=1, keepdims=True)

    prow = to_row(jnp.sum(jnp.concatenate(acc, axis=0), axis=1, keepdims=True))
    psb[...] = prow
    prb[0:1, :] = prow
    to_group(lambda o: psb, lambda r: prb.at[r : r + 1, :], as_sem.at[4], lambda r: ar_sem.at[4])

    send_halos(pq, 4)

    wait_bytes(grb.at[pl.ds(0, NZ - 1)], ar_sem.at[6])
    packed = jnp.sum(grb[...], axis=0)
    m = jnp.concatenate([packed] + [pltpu.roll(packed, 128 - 32 * t, 1) for t in range(1, 4)], axis=0)
    sub32 = lax.broadcasted_iota(jnp.int32, (32, 128), 0)
    m = jnp.where(lane32 < 32, m, (sub32 + 32 == lane32).astype(F32))
    dinv = jnp.zeros((32, 1), F32)
    sub1 = lax.broadcasted_iota(jnp.int32, (32, 1), 0)
    for k in range(K):
        r = m[k : k + 1]
        inv = 1.0 / r[:, k : k + 1]
        dinv = jnp.where(sub1 == k, inv, dinv)
        if k < K - 1:
            f = jnp.where(sub1 > k, m[:, k : k + 1] * inv, 0.0)
            m = m - f * r
    linv = jnp.where(lane32 < 32, pltpu.roll(m, 96, 1), 0.0)

    wait_bytes(prb.at[1:ngy, :], ar_sem.at[4])
    prow = jnp.sum(prb[...], axis=0, keepdims=True)
    qsb[...] = prow
    qrb[pl.ds(gx, 1), :] = prow
    to_line(qsb, qrb.at[pl.ds(gx, 1), :], as_sem.at[5], ar_sem.at[5])
    wait_halos(pq, 4)

    def sweep2(i, carry):
        sums = plane_sum(pq, i)
        for t in range(4):
            out_p[i, :, 128 * t : 128 * t + 128] = sums[t] * rv[t, i]
        return carry

    lax.fori_loop(0, 64, sweep2, 0, unroll=UNROLL)

    c_w.wait()
    wait_bytes(qrb.at[pl.ds(0, ngx - 1), :], ar_sem.at[5])
    prow = jnp.sum(qrb[...], axis=0, keepdims=True)
    y = jnp.sum(linv * prow, axis=1, keepdims=True) * dinv
    cof[...] = jnp.broadcast_to(to_col(-jnp.sum(linv * y, axis=0, keepdims=True)), (32, 128))

    for cond, dev, src, dst, there, here in faces:
        @pl.when(cond)
        def _(dev=dev, src=src, dst=dst, here=here):
            remote(src, dst, fs_sem.at[here], fr_sem.at[here], dev).wait_send()
    wait_halos_sent(pp, 0)
    wait_halos_sent(pq, 4)
    wait_bytes(srb.at[:, 1:ngy, :], as_sem.at[0])
    wait_bytes(gxb.at[pl.ds(0, 3)], as_sem.at[1])
    wait_bytes(grb.at[pl.ds(0, NZ - 1)], as_sem.at[6])
    wait_bytes(frb.at[:, 1:ngy, :], as_sem.at[2])
    wait_bytes(hrb.at[pl.ds(0, ngx - 1)], as_sem.at[3])
    wait_bytes(prb.at[1:ngy, :], as_sem.at[4])
    wait_bytes(qrb.at[pl.ds(0, ngx - 1), :], as_sem.at[5])


def finish(p_new, ww, xs, occ, cof, out_p, out_c, outc, sem):
    c_p = pltpu.make_async_copy(p_new, out_p, sem.at[0])
    c_p.start()
    cb = [cof[8 * k : 8 * k + 8, :] for k in range(4)]
    for h in range(24):
        lanes = slice(128 * h, 128 * h + 128)
        half = slice(128 * (h % 2), 128 * (h % 2) + 128)
        for c in range(3):
            u = cb[0] * ww[c, 0:8, lanes] + cb[1] * ww[c, 8:16, lanes]
            u = u + (cb[2] * ww[c, 16:24, lanes] + cb[3] * ww[c, 24:32, lanes])
            u = jnp.sum(u, axis=0, keepdims=True)
            r = 16 * c + h // 2
            outc[c : c + 1, lanes] = occ[r : r + 1, half] * (xs[r : r + 1, half] + u)
    c_c = pltpu.make_async_copy(outc, out_c, sem.at[1])
    c_c.start()
    c_p.wait()
    c_c.wait()


def shards(
    ngx, ngy,
    pressure, divergence, diagonal, normals, traction, slot_of, counts, previous, secant_v, secant_w,
):
    v = jnp.transpose(secant_v, (1, 0, 2))
    w = jnp.transpose(secant_w, (1, 0, 2))
    def in_hbm(x):
        return pltpu.with_memory_space_constraint(x, pltpu.HBM)

    hbm = pl.BlockSpec(memory_space=pltpu.HBM)
    vmem = pl.BlockSpec(memory_space=pltpu.VMEM)
    vm = pltpu.VMEM
    dma = pltpu.SemaphoreType.DMA
    p_new, w_in, own, occ, coef = pl.pallas_call(
        functools.partial(kernel, ngx, ngy),
        out_shape=(
            jax.ShapeDtypeStruct(pressure.shape, F32),
            jax.ShapeDtypeStruct(w.shape, F32),
            jax.ShapeDtypeStruct((48, 256), F32),
            jax.ShapeDtypeStruct((48, 256), F32),
            jax.ShapeDtypeStruct((32, 128), F32),
        ),
        in_specs=[hbm] * 6 + [pl.BlockSpec(memory_space=pltpu.SMEM)] + [hbm] * 3,
        out_specs=(vmem,) * 5,
        scratch_shapes=[
            vm((4, 66, 32, 128), F32),
            vm((4, 66, 32, 128), F32),
            vm((4, 64, 16, 128), F32),
            vm((4, 64, 16, 128), F32),
            vm((4, 64, 16, 128), F32),
                vm((3, 32, 3072), F32),
            vm((3, 1024), F32),
            vm((3, 1024), F32),
            vm((1, 1024), jnp.int32),
                vm((3, 3072), F32),
                vm((8, 1024), F32),
            vm((4, 8, 1024), F32),
            vm((32, 1024), F32),
            vm((128, 1024), BF16),
            vm((16, 128 * ngy), F32),
            vm((256, 128 * ngy), BF16),
            vm((144, 128 * ngy), BF16),
            vm((2, 8, 1024), F32),
            vm((2, 8, 128), F32),
            vm((4, 8, 128), F32),
            vm((2, 32, 128), F32),
            vm((2, 32, 128), F32),
            vm((3, 32, 128), F32),
            vm((3, 32, 128), F32),
            vm((144, 256), F32),
            vm((48, 256), F32),
            vm((32, 128), F32),
            vm((8, 128), F32),
            vm((4, 8, 128), F32),
            vm((8, 128), F32),
            vm((ngy // 4, 8, 128), F32),
            vm((8, 128), F32),
            vm((ngx, 8, 128), F32),
            vm((1, 128), F32),
            vm((ngy, 128), F32),
            vm((1, 128), F32),
            vm((ngx, 128), F32),
            dma((24,)),
            dma((8,)),
            dma((8,)),
            dma((8,)),
            dma((8,)),
            dma((7,)),
            dma((7,)),
            dma((4,)),
            dma((4,)),
            pltpu.SemaphoreType.REGULAR((2,)),
        ],
        compiler_params=pltpu.CompilerParams(
            collective_id=0, has_side_effects=True, vmem_limit_bytes=48 * 1024 * 1024
        ),
    )(
        in_hbm(pressure), in_hbm(divergence), in_hbm(diagonal), in_hbm(normals), in_hbm(traction), in_hbm(slot_of),
        counts, in_hbm(previous), in_hbm(v), in_hbm(w),
    )
    return pl.pallas_call(
        finish,
        out_shape=(
            jax.ShapeDtypeStruct(pressure.shape, F32),
            jax.ShapeDtypeStruct(previous.shape, F32),
        ),
        in_specs=[vmem] * 5,
        out_specs=(hbm, hbm),
        scratch_shapes=[vm((3, 3072), F32), dma((2,))],
        compiler_params=pltpu.CompilerParams(vmem_limit_bytes=4 * 1024 * 1024),
    )(p_new, w_in, own, occ, coef)


def solution(mesh):
    placed = (
        P("gx", "gy", None),
        P("gx", "gy", None),
        P("gx", "gy", None),
        P(None, ("gx", "gy")),
        P(None, ("gx", "gy")),
        P("gx", None),
        P(("gx", "gy")),
        P(None, ("gx", "gy")),
        P(None, None, ("gx", "gy")),
        P(None, None, ("gx", "gy")),
    )
    return jax.shard_map(
        functools.partial(shards, mesh.shape["gx"], mesh.shape["gy"]),
        mesh=mesh,
        in_specs=placed,
        out_specs=(P("gx", "gy", None), P(None, ("gx", "gy"))),
        check_vma=False,
    )
```

```python
import functools

import jax
import jax.numpy as jnp
from jax import lax
from jax.experimental import pallas as pl
from jax.experimental.pallas import tpu as pltpu
from jax.sharding import PartitionSpec as P

MESH = pl.DeviceIdType.MESH
F32 = jnp.float32
BF16 = jnp.bfloat16
NT = (((1,), (1,)), ((), ()))


def nt_dot(a, b):
    return lax.dot_general(a, b, NT, preferred_element_type=F32)


def split3(x):
    hi = x.astype(BF16).astype(F32)
    rest = x - hi
    mid = rest.astype(BF16).astype(F32)
    return hi, mid, rest - mid


def split2(x):
    hi = x.astype(BF16).astype(F32)
    return hi, x - hi


def kernel(
    ngx, ngy,
    p_hbm, d_hbm, g_hbm, n_hbm, t_hbm, slot_hbm, grp_hbm, prev_hbm, v_hbm, w_hbm,
    out_p, ww, xs, occ, cof,
    pp, pq, dv, gd, rv, vv, nrm, trc, slt, grp, prv,
    slab, num, ons, bt1, mh, bt2, amat,
    fj, fi, fc, ssb, srb, plc, fsb, frb, near, msk, acc0, gsb, gxb, gxs, grb, hsb, hrb, psb, prb, qsb, qrb,
    in_sem, fs_sem, fr_sem, hs_sem, hr_sem, as_sem, ar_sem, gr_sem, sl_sem, news,
):
    gx = lax.axis_index("gx")
    gy = lax.axis_index("gy")
    K = 32
    UNROLL = 4
    NEAR = 24
    CAPR = 24

    NZ, NX = ngy // 4, 4
    OFF = sorted(
        ((dz, dx) for dz in range(NZ) for dx in range(NX)),
        key=lambda o: (min(o[0], NZ - o[0]) + min(o[1], NX - o[1]), o),
    )
    gz, gq = lax.div(gy, NX), lax.rem(gy, NX)

    def peer(off):
        return lax.rem(gz + off[0], NZ) * NX + lax.rem(gq + off[1], NX)

    def wrap(i, n):
        return lax.rem(i + n, n)

    copies = []

    def load(src, dst):
        c = pltpu.make_async_copy(src, dst, in_sem.at[len(copies)])
        c.start()
        copies.append(c)
        return c

    def lanes_of(t):
        return pl.ds(128 * t, 128)

    def load_p(t):
        return load(p_hbm.at[:, :, lanes_of(t)], pp.at[t, pl.ds(1, 64), pl.ds(8, 16), :])

    c_t3 = (
        load_p(3),
        load(d_hbm.at[:, :, lanes_of(3)], dv.at[3]),
        load(g_hbm.at[:, :, lanes_of(3)], gd.at[3]),
    )
    bar = pltpu.get_barrier_semaphore()
    greet = [(wrap(gx + a, ngx), wrap(gy + b, ngy)) for a in (-1, 1) for b in (-1, 1)]
    greet += [(gx, peer(o)) for o in ((2, 0), (NZ - 2, 0), (0, 2), (1, 0), (NZ - 1, 0), (0, 1), (0, 3))]
    greet += [(gx, wrap(gy + b, ngy)) for b in (-1, 1)]
    greet += [(wrap(gx + a, ngx), gy) for a in range(1, ngx)]
    for dev in greet:
        pl.semaphore_signal(bar, inc=1, device_id=dev, device_id_type=MESH)

    c_slot = load(slot_hbm.at[:, pl.ds(pl.multiple_of(gy * 1024, 1024), 1024)], slt)
    c_p = [load_p(t) for t in range(3)]
    c_n = load(n_hbm, nrm)
    c_t = load(t_hbm, trc)
    c_grp = load(grp_hbm, grp)
    c_v = load(v_hbm, vv)
    c_dg = [load(d_hbm.at[:, :, lanes_of(t)], dv.at[t]) for t in range(3)]
    c_dg += [load(g_hbm.at[:, :, lanes_of(t)], gd.at[t]) for t in range(3)]
    c_prev = load(prev_hbm, prv)
    c_w = load(w_hbm, ww)

    has_im, has_ip = gx > 0, gx < ngx - 1
    has_jm, has_jp = gy > 0, gy < ngy - 1

    def both(a, b):
        return jnp.logical_and(a, b)

    def zero_when(cond, ref):
        @pl.when(jnp.logical_not(cond))
        def _():
            ref[...] = jnp.zeros(ref.shape, ref.dtype)

    zero_when(has_jm, fj.at[0])
    zero_when(has_jp, fj.at[1])
    zero_when(has_im, fi.at[0])
    zero_when(has_ip, fi.at[1])
    corner_has = (both(has_im, has_jm), both(has_im, has_jp), both(has_ip, has_jm), both(has_ip, has_jp))
    for k in range(4):
        zero_when(corner_has[k], fc.at[k])

    def remote(src, dst, ss, rs, dev):
        return pltpu.make_async_remote_copy(
            src_ref=src, dst_ref=dst, send_sem=ss, recv_sem=rs, device_id=dev, device_id_type=MESH
        )

    jm, jp = (gx, gy - 1), (gx, gy + 1)
    im, ip = (gx - 1, gy), (gx + 1, gy)
    lo_t, hi_t = pl.ds(0, 128), pl.ds(896, 128)
    faces = [
        (has_jm, jm, slab.at[4:8], fj.at[1, 4:8], 1, 0),
        (has_jp, jp, slab.at[4:8], fj.at[0, 4:8], 0, 1),
        (has_im, im, slab.at[4:8, lo_t], fi.at[1, 4:8], 3, 2),
        (has_ip, ip, slab.at[4:8, hi_t], fi.at[0, 4:8], 2, 3),
        (corner_has[0], (gx - 1, gy - 1), slab.at[4:8, lo_t], fc.at[3, 4:8], 7, 4),
        (corner_has[1], (gx - 1, gy + 1), slab.at[4:8, lo_t], fc.at[2, 4:8], 6, 5),
        (corner_has[2], (gx + 1, gy - 1), slab.at[4:8, hi_t], fc.at[1, 4:8], 5, 6),
        (corner_has[3], (gx + 1, gy + 1), slab.at[4:8, hi_t], fc.at[0, 4:8], 4, 7),
    ]
    face_dst = [f.at[k, 4:8] for f, n in ((fj, 2), (fi, 2), (fc, 4)) for k in range(n)]
    def to_group(src_of, dst_of, ss, rs_of):
        for r in range(ngy - 1, 0, -1):
            o = peer(OFF[r])
            remote(src_of(o), dst_of(r), ss, rs_of(r), (gx, o)).start()

    def to_line(src, dst, ss, rs):
        for d in range(1, ngx):
            remote(src, dst, ss, rs, (wrap(gx + d, ngx), gy)).start()

    def wait_bytes(ref, sem):
        pltpu.make_async_copy(ref, ref, sem).wait()

    def halos(f, base):
        return [
            (has_jm, jm, f.at[:, 1:65, 8:9, :], f.at[:, 1:65, 24:25, :], base + 1, base + 0),
            (has_jp, jp, f.at[:, 1:65, 23:24, :], f.at[:, 1:65, 7:8, :], base + 0, base + 1),
            (has_im, im, f.at[:, 1:2, 8:24, :], f.at[:, 65:66, 8:24, :], base + 3, base + 2),
            (has_ip, ip, f.at[:, 64:65, 8:24, :], f.at[:, 0:1, 8:24, :], base + 2, base + 3),
        ]

    def send_halos(f, base):
        for cond, dev, src, dst, there, here in halos(f, base):
            @pl.when(cond)
            def _(dev=dev, src=src, dst=dst, there=there, here=here):
                remote(src, dst, hs_sem.at[here], hr_sem.at[there], dev).start()

    def wait_halos(f, base):
        into = (f.at[:, 1:65, 7:8, :], f.at[:, 1:65, 24:25, :], f.at[:, 0:1, 8:24, :], f.at[:, 65:66, 8:24, :])
        for (cond, dev, src, dst, there, here), mine in zip(halos(f, base), into):
            @pl.when(cond)
            def _(dev=dev, src=src, mine=mine, here=here):
                remote(src, mine, hs_sem.at[here], hr_sem.at[here], dev).wait_recv()

    def wait_halos_sent(f, base):
        for cond, dev, src, dst, there, here in halos(f, base):
            @pl.when(cond)
            def _(dev=dev, src=src, dst=dst, there=there, here=here):
                remote(src, dst, hs_sem.at[here], hr_sem.at[here], dev).wait_send()

    for k, c in enumerate(c_t3):
        c.wait()
        for t in range(8):
            x = pp[3, 1 + 8 * t : 9 + 8 * t, 8:24, :] if k == 0 else (dv, gd)[k - 1][3, 8 * t : 8 * t + 8]
            num[k, :, 128 * t : 128 * t + 128] = x.reshape(128, 128).T[120:128]
    lane = lax.broadcasted_iota(jnp.int32, (8, 1024), 1)
    row = lax.broadcasted_iota(jnp.int32, (8, 1024), 0)
    jj = lane & 15
    P8 = num[0]
    D8 = num[1]
    R8 = 1.0 / (6.0 + num[2])

    def lateral(x):
        s = jnp.where(jj > 0, pltpu.roll(x, 1, 1), 0.0) + jnp.where(jj < 15, pltpu.roll(x, 1023, 1), 0.0)
        return s + jnp.where(lane >= 16, pltpu.roll(x, 16, 1), 0.0) + jnp.where(lane < 1008, pltpu.roll(x, 1008, 1), 0.0)

    N8 = D8 + pltpu.roll(P8, 1, 0) + jnp.where(row < 7, pltpu.roll(P8, 7, 0), 0.0) + lateral(P8)
    num[2] = R8
    num[3] = N8
    slab[...] = jnp.where(
        row >= 6, P8, jnp.where(row == 5, pltpu.roll(N8, 6, 0), pltpu.roll(R8, 5, 0))
    )

    pl.semaphore_wait(bar, len(greet))

    for cond, dev, src, dst, there, here in faces[4:] + faces[:4]:
        @pl.when(cond)
        def _(dev=dev, src=src, dst=dst, there=there, here=here):
            remote(src, dst, fs_sem.at[here], fr_sem.at[there], dev).start()

    for o in ((1, 0), (NZ - 1, 0), (2, 0), (NZ - 2, 0)):
        pl.semaphore_signal(news.at[0], inc=1, device_id=(gx, peer(o)), device_id_type=MESH)

    c_slot.wait()
    slot = slt[...].astype(F32)
    owner = jnp.floor((slot + 0.5) * (1.0 / 3072.0))
    place = slot - owner * 3072.0
    place_hi = jnp.floor((place + 0.5) * (1.0 / 256.0))
    place_lo = place - place_hi * 256.0
    oidx = lax.broadcasted_iota(jnp.int32, (32, 1024), 0).astype(F32)
    onehot = (oidx == owner).astype(F32)
    ons[...] = onehot
    upper = (
        lax.broadcasted_iota(jnp.int32, (128, 128), 0) > lax.broadcasted_iota(jnp.int32, (128, 128), 1)
    ).astype(BF16)
    ones = jnp.ones((128, 128), BF16)
    parts = [onehot[:, 128 * t : 128 * t + 128] for t in range(8)]
    stack = jnp.concatenate(parts, axis=0).astype(BF16)
    before = nt_dot(stack, upper)
    total = nt_dot(stack, ones)
    carry = jnp.zeros((32, 128), F32)
    ridx = lax.broadcasted_iota(jnp.int32, (128, 128), 0).astype(F32)
    for t in range(8):
        rank = jnp.sum(parts[t] * (before[32 * t : 32 * t + 32] + carry), axis=0, keepdims=True)
        carry = carry + total[32 * t : 32 * t + 32]
        bt1[:, 128 * t : 128 * t + 128] = (ridx == rank).astype(BF16)
    a2 = jnp.concatenate([onehot * place_hi, onehot * place_lo], axis=0).astype(BF16)
    sent = nt_dot(a2, bt1[...])
    ssb[...] = sent[:32] * 256.0 + sent[32:]
    srb[0:1, :] = ssb[pl.ds(gy, 1), :]
    fsb[pl.ds(3, 32, stride=4), :] = jnp.zeros((32, 128), F32)


    for c in c_p:
        c.wait()
    send_halos(pp, 0)

    for f in (pp, pq):
        zero_when(has_im, f.at[:, 0:1, 8:24, :])
        zero_when(has_ip, f.at[:, 65:66, 8:24, :])
        zero_when(has_jm, f.at[:, 1:65, 7:8, :])
        zero_when(has_jp, f.at[:, 1:65, 24:25, :])
    c_v.wait()
    c_grp.wait()
    first_place = gy * 3072
    mine = jnp.logical_and(grp[...] >= first_place, grp[...] < first_place + 3072).astype(F32)
    mine = mine.reshape(ngy, 8, 128)
    count = jnp.sum(jnp.sum(jnp.sum(mine, axis=0), axis=0, keepdims=True), axis=1, keepdims=True)
    gram = jnp.zeros((96, 128), F32)
    for c in range(3):
        for q in range(6):
            lo = 512 * q
            keep = (lax.broadcasted_iota(jnp.int32, (K, 512), 1) + lo).astype(F32) < count
            x = jnp.where(keep, vv[c, :, lo : lo + 512], 0.0)
            hi, mid, low = split3(x)
            s = jnp.concatenate([hi, mid, low, jnp.zeros_like(hi)], axis=0).astype(BF16)
            gram = gram + nt_dot(s[:96], s)
    gram = gram[0:32] + gram[32:64] + gram[64:96]
    gram = gram + pltpu.roll(gram, 96, 1) + pltpu.roll(gram, 64, 1)
    lane32 = lax.broadcasted_iota(jnp.int32, (32, 128), 1)
    gram = jnp.where(lane32 < 32, gram, 0.0)
    packed = gram[0:8]
    for t in range(1, 4):
        packed = packed + pltpu.roll(gram[8 * t : 8 * t + 8], 32 * t, 1)
    gsb[...] = packed
    hrb[pl.ds(gx, 1)] = packed[None]
    to_line(gsb, hrb.at[gx], as_sem.at[3], ar_sem.at[3])

    pl.semaphore_wait(news.at[0], 4)
    for o in ((2, 0), (NZ - 2, 0)):
        pl.semaphore_signal(news.at[1], inc=1, device_id=(gx, peer(o)), device_id_type=MESH)

    for c in c_dg:
        c.wait()

    def recip(i, carry):
        for t in range(4):
            rv[t, i] = 1.0 / (6.0 + gd[t, i])
        return carry

    lax.fori_loop(0, 64, recip, 0, unroll=4)

    pl.semaphore_wait(news.at[1], 2)
    to_group(lambda o: ssb.at[pl.ds(o, 1), :], lambda r: srb.at[r : r + 1, :], as_sem.at[0], lambda r: sl_sem.at[int(r >= NEAR)])

    for (cond, dev, src, dst, there, here), mine in zip(faces, face_dst):
        @pl.when(cond)
        def _(dev=dev, src=src, mine=mine, here=here):
            remote(src, mine, fs_sem.at[here], fr_sem.at[here], dev).wait_recv()
    a_jm = jnp.where(jj == 0, pltpu.roll(fj[0], 1009, 1), 0.0)
    a_jp = jnp.where(jj == 15, pltpu.roll(fj[1], 15, 1), 0.0)
    lane1 = lax.broadcasted_iota(jnp.int32, (8, 128), 1)
    gap = jnp.zeros((8, 768), F32)
    a_i = jnp.concatenate(
        [
            jnp.where(lane1 < 16, pltpu.roll(fi[0], 16, 1), 0.0),
            gap,
            jnp.where(lane1 >= 112, pltpu.roll(fi[1], 112, 1), 0.0),
        ],
        axis=1,
    )
    corner = jnp.concatenate(
        [
            jnp.where(lane1 == 0, pltpu.roll(fc[0], 1, 1), 0.0)
            + jnp.where(lane1 == 15, pltpu.roll(fc[1], 31, 1), 0.0),
            gap,
            jnp.where(lane1 == 112, pltpu.roll(fc[2], 97, 1), 0.0)
            + jnp.where(lane1 == 127, pltpu.roll(fc[3], 127, 1), 0.0),
        ],
        axis=1,
    )
    P8 = num[0]
    D8 = num[1]
    R8 = num[2]
    once = (num[3] + a_jm + a_jp + a_i) * R8
    base = P8[7:8] + corner[7:8]
    beyond = (
        (a_jm[5:6] + base) * a_jm[4:5] + (a_jp[5:6] + base) * a_jp[4:5] + (a_i[5:6] + base) * a_i[4:5]
    )
    surface = (D8[7:8] + once[6:7] + lateral(once)[7:8] + beyond) * R8[7:8]
    c_n.wait()
    c_t.wait()
    forces = nrm[...] * surface + trc[...]

    onehot = ons[...]
    rows = []
    for piece in split2(forces):
        for c in range(3):
            rows.append((onehot * piece[c : c + 1]).astype(BF16))
    moved = nt_dot(jnp.concatenate(rows, axis=0), bt1[...])
    moved = moved[0:96] + moved[96:192]
    for c in range(3):
        fsb[pl.ds(c, 32, stride=4), :] = moved[32 * c : 32 * c + 32]
    frb[0:4, :] = fsb[pl.ds(pl.multiple_of(4 * gy, 4), 4), :]
    to_group(lambda o: fsb.at[pl.ds(pl.multiple_of(4 * o, 4), 4), :], lambda r: frb.at[4 * r : 4 * r + 4, :], as_sem.at[2], lambda r: gr_sem.at[int(r >= NEAR)])

    def slot_row(ref, c, h):
        return ref[16 * c + h // 2 : 16 * c + h // 2 + 1, 128 * (h % 2) : 128 * (h % 2) + 128]

    where = lax.broadcasted_iota(jnp.int32, (48, 256), 0)
    where = (where & 15) * 256 + lax.broadcasted_iota(jnp.int32, (48, 256), 1)
    occ[...] = (where.astype(F32) < count).astype(F32)
    c_prev.wait()
    acc = [jnp.zeros((8, 128), F32) for _ in range(4)]
    for h in range(CAPR):
        lanes = slice(128 * h, 128 * h + 128)
        for c in range(3):
            res = slot_row(occ, c, h) * prv[c : c + 1, lanes]
            for k in range(4):
                acc[k] = acc[k] - vv[c, 8 * k : 8 * k + 8, lanes] * res
    for k in range(4):
        acc0[8 * k : 8 * k + 8] = acc[k]

    wait_bytes(hrb.at[pl.ds(0, ngx - 1)], ar_sem.at[3])
    packed = jnp.sum(hrb[...], axis=0)
    hsb[...] = packed
    gxb[pl.ds(gq, 1)] = packed[None]
    for d in (2, 1, 3):
        remote(hsb, gxb.at[gq], as_sem.at[1], ar_sem.at[1], (gx, gz * NX + wrap(gq + d, NX))).start()

    lane2 = lax.broadcasted_iota(jnp.int32, (16, 128), 1)

    def plane_sum(f, i):
        xs_ = [f[t, i + 1, 8:24, :] for t in range(4)]
        rr = [pltpu.roll(x, 1, 1) for x in xs_]
        rl = [pltpu.roll(x, 127, 1) for x in xs_]
        zero = jnp.zeros((16, 128), F32)
        res = []
        for t in range(4):
            down = jnp.where(lane2 == 0, rr[t - 1] if t > 0 else zero, rr[t])
            up = jnp.where(lane2 == 127, rl[t + 1] if t < 3 else zero, rl[t])
            s = f[t, i, 8:24, :] + f[t, i + 2, 8:24, :]
            s = s + (f[t, i + 1, 7:23, :] + f[t, i + 1, 9:25, :])
            res.append(dv[t, i] + s + (up + down))
        return res

    wait_halos(pp, 0)

    def sweep1(i, carry):
        sums = plane_sum(pp, i)
        for t in range(4):
            pq[t, i + 1, 8:24, :] = sums[t] * rv[t, i]
        return carry

    lax.fori_loop(0, 64, sweep1, 0, unroll=UNROLL)


    wait_bytes(gxb.at[pl.ds(0, 3)], ar_sem.at[1])
    packed = jnp.sum(gxb[...], axis=0)
    gxs[...] = packed
    grb[pl.ds(gz, 1)] = packed[None]
    for d in range(NZ - 1, 0, -1):
        e = (d + 1) // 2 if d % 2 else NZ - d // 2
        remote(gxs, grb.at[gz], as_sem.at[6], ar_sem.at[6], (gx, wrap(gz + e, NZ) * NX + gq)).start()

    hidx = lax.broadcasted_iota(jnp.int32, (16, 128), 0).astype(F32)
    lidx = [(lax.broadcasted_iota(jnp.int32, (16, 128), 0) + 16 * k).astype(F32).astype(BF16) for k in range(16)]
    one, zero = jnp.ones((16, 128), BF16), jnp.zeros((16, 128), BF16)

    def masks(g, lo, hi):
        wait_bytes(srb.at[max(lo, 1) : hi, :], sl_sem.at[g])
        place = srb[lo:hi, :]
        place_hi = jnp.floor((place + 0.5) * (1.0 / 256.0))
        plc[0, lo:hi, :] = place_hi
        plc[1, lo:hi, :] = place - place_hi * 256.0
        for b in range(lo, hi):
            lanes = slice(128 * b, 128 * b + 128)
            mh[:, lanes] = (hidx == plc[0, b : b + 1, :]).astype(F32)
            low = jnp.broadcast_to(plc[1, b : b + 1, :], (16, 128)).astype(BF16)
            for k in range(16):
                bt2[16 * k : 16 * k + 16, lanes] = jnp.where(lidx[k] == low, one, zero)

    def place(g, lo, hi):
        wait_bytes(frb.at[4 * max(lo, 1) : 4 * hi, :], gr_sem.at[g])
        for c in range(3):
            for b0 in range(lo, hi, 8):
                pieces = split2(frb[pl.ds(4 * b0 + c, 8, stride=4), :])
                for b in range(8):
                    lanes = slice(128 * (b0 + b), 128 * (b0 + b) + 128)
                    m = mh[:, lanes]
                    for k in range(2):
                        r0 = 48 * k + 16 * c
                        amat[r0 : r0 + 16, lanes] = (m * pieces[k][b : b + 1]).astype(BF16)
        lanes = slice(128 * lo, 128 * hi)
        return nt_dot(amat[:, lanes], bt2[:, lanes])

    masks(0, 0, NEAR)
    masks(1, NEAR, ngy)
    near[...] = place(0, 0, NEAR)

    own = near[...] + place(1, NEAR, ngy)
    own = own[0:48] + own[48:96]
    xs[...] = own
    msk[...] = own * occ[...]
    acc = [acc0[8 * k : 8 * k + 8] for k in range(4)]
    for h in range(CAPR):
        lanes = slice(128 * h, 128 * h + 128)
        for c in range(3):
            res = slot_row(msk, c, h)
            for k in range(4):
                acc[k] = acc[k] + vv[c, 8 * k : 8 * k + 8, lanes] * res
    diag = lax.broadcasted_iota(jnp.int32, (32, 128), 0) == lane32

    def to_row(col):
        return jnp.sum(jnp.where(diag, col, 0.0), axis=0, keepdims=True)

    def to_col(r):
        return jnp.sum(jnp.where(diag, r, 0.0), axis=1, keepdims=True)

    prow = to_row(jnp.sum(jnp.concatenate(acc, axis=0), axis=1, keepdims=True))
    psb[...] = prow
    prb[0:1, :] = prow
    to_group(lambda o: psb, lambda r: prb.at[r : r + 1, :], as_sem.at[4], lambda r: ar_sem.at[4])

    send_halos(pq, 4)

    wait_bytes(grb.at[pl.ds(0, NZ - 1)], ar_sem.at[6])
    packed = jnp.sum(grb[...], axis=0)
    m = jnp.concatenate([packed] + [pltpu.roll(packed, 128 - 32 * t, 1) for t in range(1, 4)], axis=0)
    sub32 = lax.broadcasted_iota(jnp.int32, (32, 128), 0)
    m = jnp.where(lane32 < 32, m, (sub32 + 32 == lane32).astype(F32))
    dinv = jnp.zeros((32, 1), F32)
    sub1 = lax.broadcasted_iota(jnp.int32, (32, 1), 0)
    for k in range(K):
        r = m[k : k + 1]
        inv = 1.0 / r[:, k : k + 1]
        dinv = jnp.where(sub1 == k, inv, dinv)
        if k < K - 1:
            f = jnp.where(sub1 > k, m[:, k : k + 1] * inv, 0.0)
            m = m - f * r
    linv = jnp.where(lane32 < 32, pltpu.roll(m, 96, 1), 0.0)

    wait_bytes(prb.at[1:ngy, :], ar_sem.at[4])
    prow = jnp.sum(prb[...], axis=0, keepdims=True)
    qsb[...] = prow
    qrb[pl.ds(gx, 1), :] = prow
    to_line(qsb, qrb.at[pl.ds(gx, 1), :], as_sem.at[5], ar_sem.at[5])
    wait_halos(pq, 4)

    def sweep2(i, carry):
        sums = plane_sum(pq, i)
        for t in range(4):
            out_p[i, :, 128 * t : 128 * t + 128] = sums[t] * rv[t, i]
        return carry

    lax.fori_loop(0, 64, sweep2, 0, unroll=UNROLL)

    c_w.wait()
    wait_bytes(qrb.at[pl.ds(0, ngx - 1), :], ar_sem.at[5])
    prow = jnp.sum(qrb[...], axis=0, keepdims=True)
    y = jnp.sum(linv * prow, axis=1, keepdims=True) * dinv
    cof[...] = jnp.broadcast_to(to_col(-jnp.sum(linv * y, axis=0, keepdims=True)), (32, 128))

    for cond, dev, src, dst, there, here in faces:
        @pl.when(cond)
        def _(dev=dev, src=src, dst=dst, here=here):
            remote(src, dst, fs_sem.at[here], fr_sem.at[here], dev).wait_send()
    wait_halos_sent(pp, 0)
    wait_halos_sent(pq, 4)
    wait_bytes(srb.at[1:ngy, :], as_sem.at[0])
    wait_bytes(gxb.at[pl.ds(0, 3)], as_sem.at[1])
    wait_bytes(grb.at[pl.ds(0, NZ - 1)], as_sem.at[6])
    wait_bytes(frb.at[4 : 4 * ngy, :], as_sem.at[2])
    wait_bytes(hrb.at[pl.ds(0, ngx - 1)], as_sem.at[3])
    wait_bytes(prb.at[1:ngy, :], as_sem.at[4])
    wait_bytes(qrb.at[pl.ds(0, ngx - 1), :], as_sem.at[5])


def finish(p_new, ww, xs, occ, cof, out_p, out_c, outc, sem):
    c_p = pltpu.make_async_copy(p_new, out_p, sem.at[0])
    c_p.start()
    cb = [cof[8 * k : 8 * k + 8, :] for k in range(4)]
    for h in range(24):
        lanes = slice(128 * h, 128 * h + 128)
        half = slice(128 * (h % 2), 128 * (h % 2) + 128)
        for c in range(3):
            u = cb[0] * ww[c, 0:8, lanes] + cb[1] * ww[c, 8:16, lanes]
            u = u + (cb[2] * ww[c, 16:24, lanes] + cb[3] * ww[c, 24:32, lanes])
            u = jnp.sum(u, axis=0, keepdims=True)
            r = 16 * c + h // 2
            outc[c : c + 1, lanes] = occ[r : r + 1, half] * (xs[r : r + 1, half] + u)
    c_c = pltpu.make_async_copy(outc, out_c, sem.at[1])
    c_c.start()
    c_p.wait()
    c_c.wait()


def shards(
    ngx, ngy,
    pressure, divergence, diagonal, normals, traction, slot_of, counts, previous, secant_v, secant_w,
):
    v = jnp.transpose(secant_v, (1, 0, 2))
    w = jnp.transpose(secant_w, (1, 0, 2))
    def in_hbm(x):
        return pltpu.with_memory_space_constraint(x, pltpu.HBM)

    hbm = pl.BlockSpec(memory_space=pltpu.HBM)
    vmem = pl.BlockSpec(memory_space=pltpu.VMEM)
    vm = pltpu.VMEM
    dma = pltpu.SemaphoreType.DMA
    p_new, w_in, own, occ, coef = pl.pallas_call(
        functools.partial(kernel, ngx, ngy),
        out_shape=(
            jax.ShapeDtypeStruct(pressure.shape, F32),
            jax.ShapeDtypeStruct(w.shape, F32),
            jax.ShapeDtypeStruct((48, 256), F32),
            jax.ShapeDtypeStruct((48, 256), F32),
            jax.ShapeDtypeStruct((32, 128), F32),
        ),
        in_specs=[hbm] * 10,
        out_specs=(vmem,) * 5,
        scratch_shapes=[
            vm((4, 66, 32, 128), F32),
            vm((4, 66, 32, 128), F32),
            vm((4, 64, 16, 128), F32),
            vm((4, 64, 16, 128), F32),
            vm((4, 64, 16, 128), F32),
                vm((3, 32, 3072), F32),
            vm((3, 1024), F32),
            vm((3, 1024), F32),
            vm((1, 1024), jnp.int32),
            vm((8 * ngy, 128), jnp.int32),
                vm((3, 3072), F32),
                vm((8, 1024), F32),
            vm((4, 8, 1024), F32),
            vm((32, 1024), F32),
            vm((128, 1024), BF16),
            vm((16, 128 * ngy), F32),
            vm((256, 128 * ngy), BF16),
            vm((96, 128 * ngy), BF16),
            vm((2, 8, 1024), F32),
            vm((2, 8, 128), F32),
            vm((4, 8, 128), F32),
            vm((32, 128), F32),
            vm((ngy, 128), F32),
            vm((2, ngy, 128), F32),
            vm((128, 128), F32),
            vm((128, 128), F32),
            vm((96, 256), F32),
            vm((48, 256), F32),
            vm((32, 128), F32),
            vm((8, 128), F32),
            vm((4, 8, 128), F32),
            vm((8, 128), F32),
            vm((ngy // 4, 8, 128), F32),
            vm((8, 128), F32),
            vm((ngx, 8, 128), F32),
            vm((1, 128), F32),
            vm((ngy, 128), F32),
            vm((1, 128), F32),
            vm((ngx, 128), F32),
            dma((24,)),
            dma((8,)),
            dma((8,)),
            dma((8,)),
            dma((8,)),
            dma((7,)),
            dma((7,)),
            dma((2,)),
            dma((2,)),
            pltpu.SemaphoreType.REGULAR((2,)),
        ],
        compiler_params=pltpu.CompilerParams(
            collective_id=0, has_side_effects=True, vmem_limit_bytes=48 * 1024 * 1024
        ),
    )(
        in_hbm(pressure), in_hbm(divergence), in_hbm(diagonal), in_hbm(normals), in_hbm(traction), in_hbm(slot_of),
        in_hbm(slot_of.reshape(8 * ngy, 128)), in_hbm(previous), in_hbm(v), in_hbm(w),
    )
    return pl.pallas_call(
        finish,
        out_shape=(
            jax.ShapeDtypeStruct(pressure.shape, F32),
            jax.ShapeDtypeStruct(previous.shape, F32),
        ),
        in_specs=[vmem] * 5,
        out_specs=(hbm, hbm),
        scratch_shapes=[vm((3, 3072), F32), dma((2,))],
        compiler_params=pltpu.CompilerParams(vmem_limit_bytes=4 * 1024 * 1024),
    )(p_new, w_in, own, occ, coef)


def solution(mesh):
    placed = (
        P("gx", "gy", None),
        P("gx", "gy", None),
        P("gx", "gy", None),
        P(None, ("gx", "gy")),
        P(None, ("gx", "gy")),
        P("gx", None),
        P(("gx", "gy")),
        P(None, ("gx", "gy")),
        P(None, None, ("gx", "gy")),
        P(None, None, ("gx", "gy")),
    )
    return jax.shard_map(
        functools.partial(shards, mesh.shape["gx"], mesh.shape["gy"]),
        mesh=mesh,
        in_specs=placed,
        out_specs=(P("gx", "gy", None), P(None, ("gx", "gy"))),
        check_vma=False,
    )
```

```python
import functools

import jax
import jax.numpy as jnp
from jax import lax
from jax.experimental import pallas as pl
from jax.experimental.pallas import tpu as pltpu
from jax.sharding import PartitionSpec as P

MESH = pl.DeviceIdType.MESH
F32 = jnp.float32
BF16 = jnp.bfloat16
NT = (((1,), (1,)), ((), ()))


def nt_dot(a, b):
    return lax.dot_general(a, b, NT, preferred_element_type=F32)


def split3(x):
    hi = x.astype(BF16).astype(F32)
    rest = x - hi
    mid = rest.astype(BF16).astype(F32)
    return hi, mid, rest - mid


def split2(x):
    hi = x.astype(BF16).astype(F32)
    return hi, x - hi


def kernel(
    ngx, ngy,
    p_hbm, d_hbm, g_hbm, n_hbm, t_hbm, slot_hbm, grp_hbm, prev_hbm, v_hbm, w_hbm,
    out_p, ww, xs, occ, lnv, dnv, prj,
    pp, pq, dv, gd, rv, vv, nrm, trc, slt, grp, prv,
    slab, num, ons, bt1, mh, bt2, amat,
    fj, fi, fc, ssb, srb, plc, fsb, frb, near, msk, acc0, gsb, gxb, gxs, grb, hsb, hrb, psb, prb, qsb, qrb,
    in_sem, fs_sem, fr_sem, hs_sem, hr_sem, as_sem, ar_sem, gr_sem, sl_sem, news,
):
    gx = lax.axis_index("gx")
    gy = lax.axis_index("gy")
    K = 32
    UNROLL = 4
    NEAR = 24
    CAPR = 24

    NZ, NX = ngy // 4, 4
    OFF = sorted(
        ((dz, dx) for dz in range(NZ) for dx in range(NX)),
        key=lambda o: (min(o[0], NZ - o[0]) + min(o[1], NX - o[1]), o),
    )
    gz, gq = lax.div(gy, NX), lax.rem(gy, NX)

    def peer(off):
        return lax.rem(gz + off[0], NZ) * NX + lax.rem(gq + off[1], NX)

    def wrap(i, n):
        return lax.rem(i + n, n)

    copies = []

    def load(src, dst):
        c = pltpu.make_async_copy(src, dst, in_sem.at[len(copies)])
        c.start()
        copies.append(c)
        return c

    def lanes_of(t):
        return pl.ds(128 * t, 128)

    def load_p(t):
        return load(p_hbm.at[:, :, lanes_of(t)], pp.at[t, pl.ds(1, 64), pl.ds(8, 16), :])

    c_t3 = (
        load_p(3),
        load(d_hbm.at[:, :, lanes_of(3)], dv.at[3]),
        load(g_hbm.at[:, :, lanes_of(3)], gd.at[3]),
    )
    bar = pltpu.get_barrier_semaphore()
    greet = [(wrap(gx + a, ngx), wrap(gy + b, ngy)) for a in (-1, 1) for b in (-1, 1)]
    greet += [(gx, peer(o)) for o in ((2, 0), (NZ - 2, 0), (0, 2), (1, 0), (NZ - 1, 0), (0, 1), (0, 3))]
    greet += [(gx, wrap(gy + b, ngy)) for b in (-1, 1)]
    greet += [(wrap(gx + a, ngx), gy) for a in range(1, ngx)]
    for dev in greet:
        pl.semaphore_signal(bar, inc=1, device_id=dev, device_id_type=MESH)

    c_slot = load(slot_hbm.at[:, pl.ds(pl.multiple_of(gy * 1024, 1024), 1024)], slt)
    c_p = [load_p(t) for t in range(3)]
    c_n = load(n_hbm, nrm)
    c_t = load(t_hbm, trc)
    c_grp = load(grp_hbm, grp)
    c_v = load(v_hbm, vv)
    c_dg = [load(d_hbm.at[:, :, lanes_of(t)], dv.at[t]) for t in range(3)]
    c_dg += [load(g_hbm.at[:, :, lanes_of(t)], gd.at[t]) for t in range(3)]
    c_prev = load(prev_hbm, prv)
    c_w = load(w_hbm, ww)

    has_im, has_ip = gx > 0, gx < ngx - 1
    has_jm, has_jp = gy > 0, gy < ngy - 1

    def both(a, b):
        return jnp.logical_and(a, b)

    def zero_when(cond, ref):
        @pl.when(jnp.logical_not(cond))
        def _():
            ref[...] = jnp.zeros(ref.shape, ref.dtype)

    zero_when(has_jm, fj.at[0])
    zero_when(has_jp, fj.at[1])
    zero_when(has_im, fi.at[0])
    zero_when(has_ip, fi.at[1])
    corner_has = (both(has_im, has_jm), both(has_im, has_jp), both(has_ip, has_jm), both(has_ip, has_jp))
    for k in range(4):
        zero_when(corner_has[k], fc.at[k])

    def remote(src, dst, ss, rs, dev):
        return pltpu.make_async_remote_copy(
            src_ref=src, dst_ref=dst, send_sem=ss, recv_sem=rs, device_id=dev, device_id_type=MESH
        )

    jm, jp = (gx, gy - 1), (gx, gy + 1)
    im, ip = (gx - 1, gy), (gx + 1, gy)
    lo_t, hi_t = pl.ds(0, 128), pl.ds(896, 128)
    faces = [
        (has_jm, jm, slab.at[4:8], fj.at[1, 4:8], 1, 0),
        (has_jp, jp, slab.at[4:8], fj.at[0, 4:8], 0, 1),
        (has_im, im, slab.at[4:8, lo_t], fi.at[1, 4:8], 3, 2),
        (has_ip, ip, slab.at[4:8, hi_t], fi.at[0, 4:8], 2, 3),
        (corner_has[0], (gx - 1, gy - 1), slab.at[4:8, lo_t], fc.at[3, 4:8], 7, 4),
        (corner_has[1], (gx - 1, gy + 1), slab.at[4:8, lo_t], fc.at[2, 4:8], 6, 5),
        (corner_has[2], (gx + 1, gy - 1), slab.at[4:8, hi_t], fc.at[1, 4:8], 5, 6),
        (corner_has[3], (gx + 1, gy + 1), slab.at[4:8, hi_t], fc.at[0, 4:8], 4, 7),
    ]
    face_dst = [f.at[k, 4:8] for f, n in ((fj, 2), (fi, 2), (fc, 4)) for k in range(n)]
    def to_group(src_of, dst_of, ss, rs_of):
        for r in range(ngy - 1, 0, -1):
            o = peer(OFF[r])
            remote(src_of(o), dst_of(r), ss, rs_of(r), (gx, o)).start()

    def to_line(src, dst, ss, rs):
        for d in sorted(range(1, ngx), key=lambda d: abs(2 * d - ngx)):
            remote(src, dst, ss, rs, (wrap(gx + d, ngx), gy)).start()

    def wait_bytes(ref, sem):
        pltpu.make_async_copy(ref, ref, sem).wait()

    def halos(f, base):
        return [
            (has_jm, jm, f.at[:, 1:65, 8:9, :], f.at[:, 1:65, 24:25, :], base + 1, base + 0),
            (has_jp, jp, f.at[:, 1:65, 23:24, :], f.at[:, 1:65, 7:8, :], base + 0, base + 1),
            (has_im, im, f.at[:, 1:2, 8:24, :], f.at[:, 65:66, 8:24, :], base + 3, base + 2),
            (has_ip, ip, f.at[:, 64:65, 8:24, :], f.at[:, 0:1, 8:24, :], base + 2, base + 3),
        ]

    def send_halos(f, base):
        for cond, dev, src, dst, there, here in halos(f, base):
            @pl.when(cond)
            def _(dev=dev, src=src, dst=dst, there=there, here=here):
                remote(src, dst, hs_sem.at[here], hr_sem.at[there], dev).start()

    def wait_halos(f, base):
        into = (f.at[:, 1:65, 7:8, :], f.at[:, 1:65, 24:25, :], f.at[:, 0:1, 8:24, :], f.at[:, 65:66, 8:24, :])
        for (cond, dev, src, dst, there, here), mine in zip(halos(f, base), into):
            @pl.when(cond)
            def _(dev=dev, src=src, mine=mine, here=here):
                remote(src, mine, hs_sem.at[here], hr_sem.at[here], dev).wait_recv()

    def wait_halos_sent(f, base):
        for cond, dev, src, dst, there, here in halos(f, base):
            @pl.when(cond)
            def _(dev=dev, src=src, dst=dst, there=there, here=here):
                remote(src, dst, hs_sem.at[here], hr_sem.at[here], dev).wait_send()

    for k, c in enumerate(c_t3):
        c.wait()
        for t in range(8):
            x = pp[3, 1 + 8 * t : 9 + 8 * t, 8:24, :] if k == 0 else (dv, gd)[k - 1][3, 8 * t : 8 * t + 8]
            num[k, :, 128 * t : 128 * t + 128] = x.reshape(128, 128).T[120:128]
    lane = lax.broadcasted_iota(jnp.int32, (8, 1024), 1)
    row = lax.broadcasted_iota(jnp.int32, (8, 1024), 0)
    jj = lane & 15
    P8 = num[0]
    D8 = num[1]
    R8 = 1.0 / (6.0 + num[2])

    def lateral(x):
        s = jnp.where(jj > 0, pltpu.roll(x, 1, 1), 0.0) + jnp.where(jj < 15, pltpu.roll(x, 1023, 1), 0.0)
        return s + jnp.where(lane >= 16, pltpu.roll(x, 16, 1), 0.0) + jnp.where(lane < 1008, pltpu.roll(x, 1008, 1), 0.0)

    N8 = D8 + pltpu.roll(P8, 1, 0) + jnp.where(row < 7, pltpu.roll(P8, 7, 0), 0.0) + lateral(P8)
    num[2] = R8
    num[3] = N8
    slab[...] = jnp.where(
        row >= 6, P8, jnp.where(row == 5, pltpu.roll(N8, 6, 0), pltpu.roll(R8, 5, 0))
    )

    pl.semaphore_wait(bar, len(greet))

    for cond, dev, src, dst, there, here in faces[4:] + faces[:4]:
        @pl.when(cond)
        def _(dev=dev, src=src, dst=dst, there=there, here=here):
            remote(src, dst, fs_sem.at[here], fr_sem.at[there], dev).start()

    for o in ((1, 0), (NZ - 1, 0), (2, 0), (NZ - 2, 0)):
        pl.semaphore_signal(news.at[0], inc=1, device_id=(gx, peer(o)), device_id_type=MESH)

    c_slot.wait()
    slot = slt[...].astype(F32)
    owner = jnp.floor((slot + 0.5) * (1.0 / 3072.0))
    place = slot - owner * 3072.0
    place_hi = jnp.floor((place + 0.5) * (1.0 / 256.0))
    place_lo = place - place_hi * 256.0
    oidx = lax.broadcasted_iota(jnp.int32, (32, 1024), 0).astype(F32)
    onehot = (oidx == owner).astype(F32)
    ons[...] = onehot
    upper = (
        lax.broadcasted_iota(jnp.int32, (128, 128), 0) > lax.broadcasted_iota(jnp.int32, (128, 128), 1)
    ).astype(BF16)
    ones = jnp.ones((128, 128), BF16)
    parts = [onehot[:, 128 * t : 128 * t + 128] for t in range(8)]
    stack = jnp.concatenate(parts, axis=0).astype(BF16)
    before = nt_dot(stack, upper)
    total = nt_dot(stack, ones)
    carry = jnp.zeros((32, 128), F32)
    ridx = lax.broadcasted_iota(jnp.int32, (128, 128), 0).astype(F32)
    for t in range(8):
        rank = jnp.sum(parts[t] * (before[32 * t : 32 * t + 32] + carry), axis=0, keepdims=True)
        carry = carry + total[32 * t : 32 * t + 32]
        bt1[:, 128 * t : 128 * t + 128] = (ridx == rank).astype(BF16)
    a2 = jnp.concatenate([onehot * place_hi, onehot * place_lo], axis=0).astype(BF16)
    sent = nt_dot(a2, bt1[...])
    ssb[...] = sent[:32] * 256.0 + sent[32:]
    srb[0:1, :] = ssb[pl.ds(gy, 1), :]
    fsb[pl.ds(3, 32, stride=4), :] = jnp.zeros((32, 128), F32)


    for c in c_p:
        c.wait()
    send_halos(pp, 0)

    for f in (pp, pq):
        zero_when(has_im, f.at[:, 0:1, 8:24, :])
        zero_when(has_ip, f.at[:, 65:66, 8:24, :])
        zero_when(has_jm, f.at[:, 1:65, 7:8, :])
        zero_when(has_jp, f.at[:, 1:65, 24:25, :])
    c_v.wait()
    c_grp.wait()
    first_place = gy * 3072
    mine = jnp.logical_and(grp[...] >= first_place, grp[...] < first_place + 3072).astype(F32)
    mine = mine.reshape(ngy, 8, 128)
    count = jnp.sum(jnp.sum(jnp.sum(mine, axis=0), axis=0, keepdims=True), axis=1, keepdims=True)
    gram = jnp.zeros((96, 128), F32)
    for c in range(3):
        for q in range(6):
            lo = 512 * q
            keep = (lax.broadcasted_iota(jnp.int32, (K, 512), 1) + lo).astype(F32) < count
            x = jnp.where(keep, vv[c, :, lo : lo + 512], 0.0)
            hi, mid, low = split3(x)
            s = jnp.concatenate([hi, mid, low, jnp.zeros_like(hi)], axis=0).astype(BF16)
            gram = gram + nt_dot(s[:96], s)
    gram = gram[0:32] + gram[32:64] + gram[64:96]
    gram = gram + pltpu.roll(gram, 96, 1) + pltpu.roll(gram, 64, 1)
    lane32 = lax.broadcasted_iota(jnp.int32, (32, 128), 1)
    gram = jnp.where(lane32 < 32, gram, 0.0)
    packed = gram[0:8]
    for t in range(1, 4):
        packed = packed + pltpu.roll(gram[8 * t : 8 * t + 8], 32 * t, 1)
    gsb[...] = packed
    hrb[pl.ds(gx, 1)] = packed[None]
    to_line(gsb, hrb.at[gx], as_sem.at[3], ar_sem.at[3])

    pl.semaphore_wait(news.at[0], 4)
    for o in ((2, 0), (NZ - 2, 0)):
        pl.semaphore_signal(news.at[1], inc=1, device_id=(gx, peer(o)), device_id_type=MESH)

    for c in c_dg:
        c.wait()

    def recip(i, carry):
        for t in range(4):
            rv[t, i] = 1.0 / (6.0 + gd[t, i])
        return carry

    lax.fori_loop(0, 64, recip, 0, unroll=4)

    pl.semaphore_wait(news.at[1], 2)
    to_group(lambda o: ssb.at[pl.ds(o, 1), :], lambda r: srb.at[r : r + 1, :], as_sem.at[0], lambda r: sl_sem.at[int(r >= NEAR)])

    for (cond, dev, src, dst, there, here), mine in zip(faces, face_dst):
        @pl.when(cond)
        def _(dev=dev, src=src, mine=mine, here=here):
            remote(src, mine, fs_sem.at[here], fr_sem.at[here], dev).wait_recv()
    a_jm = jnp.where(jj == 0, pltpu.roll(fj[0], 1009, 1), 0.0)
    a_jp = jnp.where(jj == 15, pltpu.roll(fj[1], 15, 1), 0.0)
    lane1 = lax.broadcasted_iota(jnp.int32, (8, 128), 1)
    gap = jnp.zeros((8, 768), F32)
    a_i = jnp.concatenate(
        [
            jnp.where(lane1 < 16, pltpu.roll(fi[0], 16, 1), 0.0),
            gap,
            jnp.where(lane1 >= 112, pltpu.roll(fi[1], 112, 1), 0.0),
        ],
        axis=1,
    )
    corner = jnp.concatenate(
        [
            jnp.where(lane1 == 0, pltpu.roll(fc[0], 1, 1), 0.0)
            + jnp.where(lane1 == 15, pltpu.roll(fc[1], 31, 1), 0.0),
            gap,
            jnp.where(lane1 == 112, pltpu.roll(fc[2], 97, 1), 0.0)
            + jnp.where(lane1 == 127, pltpu.roll(fc[3], 127, 1), 0.0),
        ],
        axis=1,
    )
    P8 = num[0]
    D8 = num[1]
    R8 = num[2]
    once = (num[3] + a_jm + a_jp + a_i) * R8
    base = P8[7:8] + corner[7:8]
    beyond = (
        (a_jm[5:6] + base) * a_jm[4:5] + (a_jp[5:6] + base) * a_jp[4:5] + (a_i[5:6] + base) * a_i[4:5]
    )
    surface = (D8[7:8] + once[6:7] + lateral(once)[7:8] + beyond) * R8[7:8]
    c_n.wait()
    c_t.wait()
    forces = nrm[...] * surface + trc[...]

    onehot = ons[...]
    rows = []
    for piece in split2(forces):
        for c in range(3):
            rows.append((onehot * piece[c : c + 1]).astype(BF16))
    moved = nt_dot(jnp.concatenate(rows, axis=0), bt1[...])
    moved = moved[0:96] + moved[96:192]
    for c in range(3):
        fsb[pl.ds(c, 32, stride=4), :] = moved[32 * c : 32 * c + 32]
    frb[0:4, :] = fsb[pl.ds(pl.multiple_of(4 * gy, 4), 4), :]
    to_group(lambda o: fsb.at[pl.ds(pl.multiple_of(4 * o, 4), 4), :], lambda r: frb.at[4 * r : 4 * r + 4, :], as_sem.at[2], lambda r: gr_sem.at[int(r >= NEAR)])

    def slot_row(ref, c, h):
        return ref[16 * c + h // 2 : 16 * c + h // 2 + 1, 128 * (h % 2) : 128 * (h % 2) + 128]

    where = lax.broadcasted_iota(jnp.int32, (48, 256), 0)
    where = (where & 15) * 256 + lax.broadcasted_iota(jnp.int32, (48, 256), 1)
    occ[...] = (where.astype(F32) < count).astype(F32)
    c_prev.wait()
    acc = [jnp.zeros((8, 128), F32) for _ in range(4)]
    for h in range(CAPR):
        lanes = slice(128 * h, 128 * h + 128)
        for c in range(3):
            res = slot_row(occ, c, h) * prv[c : c + 1, lanes]
            for k in range(4):
                acc[k] = acc[k] - vv[c, 8 * k : 8 * k + 8, lanes] * res
    for k in range(4):
        acc0[8 * k : 8 * k + 8] = acc[k]

    wait_bytes(hrb.at[pl.ds(0, ngx - 1)], ar_sem.at[3])
    packed = jnp.sum(hrb[...], axis=0)
    hsb[...] = packed
    gxb[pl.ds(gq, 1)] = packed[None]
    for d in (2, 1, 3):
        remote(hsb, gxb.at[gq], as_sem.at[1], ar_sem.at[1], (gx, gz * NX + wrap(gq + d, NX))).start()

    lane2 = lax.broadcasted_iota(jnp.int32, (16, 128), 1)

    def plane_sum(f, i):
        xs_ = [f[t, i + 1, 8:24, :] for t in range(4)]
        rr = [pltpu.roll(x, 1, 1) for x in xs_]
        rl = [pltpu.roll(x, 127, 1) for x in xs_]
        zero = jnp.zeros((16, 128), F32)
        res = []
        for t in range(4):
            down = jnp.where(lane2 == 0, rr[t - 1] if t > 0 else zero, rr[t])
            up = jnp.where(lane2 == 127, rl[t + 1] if t < 3 else zero, rl[t])
            s = f[t, i, 8:24, :] + f[t, i + 2, 8:24, :]
            s = s + (f[t, i + 1, 7:23, :] + f[t, i + 1, 9:25, :])
            res.append(dv[t, i] + s + (up + down))
        return res

    wait_halos(pp, 0)

    def sweep1(i, carry):
        sums = plane_sum(pp, i)
        for t in range(4):
            pq[t, i + 1, 8:24, :] = sums[t] * rv[t, i]
        return carry

    lax.fori_loop(0, 64, sweep1, 0, unroll=UNROLL)


    wait_bytes(gxb.at[pl.ds(0, 3)], ar_sem.at[1])
    packed = jnp.sum(gxb[...], axis=0)
    gxs[...] = packed
    grb[pl.ds(gz, 1)] = packed[None]
    for d in range(NZ - 1, 0, -1):
        e = (d + 1) // 2 if d % 2 else NZ - d // 2
        remote(gxs, grb.at[gz], as_sem.at[6], ar_sem.at[6], (gx, wrap(gz + e, NZ) * NX + gq)).start()

    hidx = lax.broadcasted_iota(jnp.int32, (16, 128), 0).astype(F32)
    lidx = [(lax.broadcasted_iota(jnp.int32, (16, 128), 0) + 16 * k).astype(F32).astype(BF16) for k in range(16)]
    one, zero = jnp.ones((16, 128), BF16), jnp.zeros((16, 128), BF16)

    def masks(g, lo, hi):
        wait_bytes(srb.at[max(lo, 1) : hi, :], sl_sem.at[g])
        place = srb[lo:hi, :]
        place_hi = jnp.floor((place + 0.5) * (1.0 / 256.0))
        plc[0, lo:hi, :] = place_hi
        plc[1, lo:hi, :] = place - place_hi * 256.0
        for b in range(lo, hi):
            lanes = slice(128 * b, 128 * b + 128)
            mh[:, lanes] = (hidx == plc[0, b : b + 1, :]).astype(F32)
            low = jnp.broadcast_to(plc[1, b : b + 1, :], (16, 128)).astype(BF16)
            for k in range(16):
                bt2[16 * k : 16 * k + 16, lanes] = jnp.where(lidx[k] == low, one, zero)

    def place(g, lo, hi):
        wait_bytes(frb.at[4 * max(lo, 1) : 4 * hi, :], gr_sem.at[g])
        for c in range(3):
            for b0 in range(lo, hi, 8):
                pieces = split2(frb[pl.ds(4 * b0 + c, 8, stride=4), :])
                for b in range(8):
                    lanes = slice(128 * (b0 + b), 128 * (b0 + b) + 128)
                    m = mh[:, lanes]
                    for k in range(2):
                        r0 = 48 * k + 16 * c
                        amat[r0 : r0 + 16, lanes] = (m * pieces[k][b : b + 1]).astype(BF16)
        lanes = slice(128 * lo, 128 * hi)
        return nt_dot(amat[:, lanes], bt2[:, lanes])

    masks(0, 0, NEAR)
    masks(1, NEAR, ngy)
    near[...] = place(0, 0, NEAR)

    own = near[...] + place(1, NEAR, ngy)
    own = own[0:48] + own[48:96]
    xs[...] = own
    msk[...] = own * occ[...]
    acc = [acc0[8 * k : 8 * k + 8] for k in range(4)]
    for h in range(CAPR):
        lanes = slice(128 * h, 128 * h + 128)
        for c in range(3):
            res = slot_row(msk, c, h)
            for k in range(4):
                acc[k] = acc[k] + vv[c, 8 * k : 8 * k + 8, lanes] * res
    diag = lax.broadcasted_iota(jnp.int32, (32, 128), 0) == lane32

    def to_row(col):
        return jnp.sum(jnp.where(diag, col, 0.0), axis=0, keepdims=True)

    prow = to_row(jnp.sum(jnp.concatenate(acc, axis=0), axis=1, keepdims=True))
    psb[...] = prow
    prb[0:1, :] = prow
    to_group(lambda o: psb, lambda r: prb.at[r : r + 1, :], as_sem.at[4], lambda r: ar_sem.at[4])

    send_halos(pq, 4)

    wait_bytes(grb.at[pl.ds(0, NZ - 1)], ar_sem.at[6])
    packed = jnp.sum(grb[...], axis=0)
    m = jnp.concatenate([packed] + [pltpu.roll(packed, 128 - 32 * t, 1) for t in range(1, 4)], axis=0)
    sub32 = lax.broadcasted_iota(jnp.int32, (32, 128), 0)
    m = jnp.where(lane32 < 32, m, (sub32 + 32 == lane32).astype(F32))
    dinv = jnp.zeros((32, 1), F32)
    sub1 = lax.broadcasted_iota(jnp.int32, (32, 1), 0)
    for k in range(K):
        r = m[k : k + 1]
        inv = 1.0 / r[:, k : k + 1]
        dinv = jnp.where(sub1 == k, inv, dinv)
        if k < K - 1:
            f = jnp.where(sub1 > k, m[:, k : k + 1] * inv, 0.0)
            m = m - f * r
    lnv[...] = jnp.where(lane32 < 32, pltpu.roll(m, 96, 1), 0.0)
    dnv[...] = jnp.broadcast_to(dinv, (32, 128))

    wait_bytes(prb.at[1:ngy, :], ar_sem.at[4])
    prow = jnp.sum(prb[...], axis=0, keepdims=True)
    qsb[...] = prow
    qrb[pl.ds(gx, 1), :] = prow
    to_line(qsb, qrb.at[pl.ds(gx, 1), :], as_sem.at[5], ar_sem.at[5])
    wait_halos(pq, 4)

    def sweep2(i, carry):
        sums = plane_sum(pq, i)
        for t in range(4):
            out_p[i, :, 128 * t : 128 * t + 128] = sums[t] * rv[t, i]
        return carry

    lax.fori_loop(0, 64, sweep2, 0, unroll=UNROLL)

    c_w.wait()
    wait_bytes(qrb.at[pl.ds(0, ngx - 1), :], ar_sem.at[5])
    prj[...] = qrb[...]

    for cond, dev, src, dst, there, here in faces:
        @pl.when(cond)
        def _(dev=dev, src=src, dst=dst, here=here):
            remote(src, dst, fs_sem.at[here], fr_sem.at[here], dev).wait_send()
    wait_halos_sent(pp, 0)
    wait_halos_sent(pq, 4)
    wait_bytes(srb.at[1:ngy, :], as_sem.at[0])
    wait_bytes(gxb.at[pl.ds(0, 3)], as_sem.at[1])
    wait_bytes(grb.at[pl.ds(0, NZ - 1)], as_sem.at[6])
    wait_bytes(frb.at[4 : 4 * ngy, :], as_sem.at[2])
    wait_bytes(hrb.at[pl.ds(0, ngx - 1)], as_sem.at[3])
    wait_bytes(prb.at[1:ngy, :], as_sem.at[4])
    wait_bytes(qrb.at[pl.ds(0, ngx - 1), :], as_sem.at[5])


def finish(p_new, ww, xs, occ, lnv, dnv, prj, out_p, out_c, outc, sem):
    c_p = pltpu.make_async_copy(p_new, out_p, sem.at[0])
    c_p.start()
    linv = lnv[...]
    prow = jnp.sum(prj[...], axis=0, keepdims=True)
    y = jnp.sum(linv * prow, axis=1, keepdims=True) * dnv[...]
    crow = -jnp.sum(linv * y, axis=0, keepdims=True)
    diag = lax.broadcasted_iota(jnp.int32, (32, 128), 0) == lax.broadcasted_iota(jnp.int32, (32, 128), 1)
    coef = jnp.broadcast_to(jnp.sum(jnp.where(diag, crow, 0.0), axis=1, keepdims=True), (32, 128))
    cb = [coef[8 * k : 8 * k + 8, :] for k in range(4)]
    for h in range(24):
        lanes = slice(128 * h, 128 * h + 128)
        half = slice(128 * (h % 2), 128 * (h % 2) + 128)
        for c in range(3):
            u = cb[0] * ww[c, 0:8, lanes] + cb[1] * ww[c, 8:16, lanes]
            u = u + (cb[2] * ww[c, 16:24, lanes] + cb[3] * ww[c, 24:32, lanes])
            u = jnp.sum(u, axis=0, keepdims=True)
            r = 16 * c + h // 2
            outc[c : c + 1, lanes] = occ[r : r + 1, half] * (xs[r : r + 1, half] + u)
    c_c = pltpu.make_async_copy(outc, out_c, sem.at[1])
    c_c.start()
    c_p.wait()
    c_c.wait()


def shards(
    ngx, ngy,
    pressure, divergence, diagonal, normals, traction, slot_of, counts, previous, secant_v, secant_w,
):
    v = jnp.transpose(secant_v, (1, 0, 2))
    w = jnp.transpose(secant_w, (1, 0, 2))
    def in_hbm(x):
        return pltpu.with_memory_space_constraint(x, pltpu.HBM)

    hbm = pl.BlockSpec(memory_space=pltpu.HBM)
    vmem = pl.BlockSpec(memory_space=pltpu.VMEM)
    vm = pltpu.VMEM
    dma = pltpu.SemaphoreType.DMA
    p_new, *rest = pl.pallas_call(
        functools.partial(kernel, ngx, ngy),
        out_shape=(
            jax.ShapeDtypeStruct(pressure.shape, F32),
            jax.ShapeDtypeStruct(w.shape, F32),
            jax.ShapeDtypeStruct((48, 256), F32),
            jax.ShapeDtypeStruct((48, 256), F32),
            jax.ShapeDtypeStruct((32, 128), F32),
            jax.ShapeDtypeStruct((32, 128), F32),
            jax.ShapeDtypeStruct((ngx, 128), F32),
        ),
        in_specs=[hbm] * 10,
        out_specs=(vmem,) * 7,
        scratch_shapes=[
            vm((4, 66, 32, 128), F32),
            vm((4, 66, 32, 128), F32),
            vm((4, 64, 16, 128), F32),
            vm((4, 64, 16, 128), F32),
            vm((4, 64, 16, 128), F32),
                vm((3, 32, 3072), F32),
            vm((3, 1024), F32),
            vm((3, 1024), F32),
            vm((1, 1024), jnp.int32),
            vm((8 * ngy, 128), jnp.int32),
                vm((3, 3072), F32),
                vm((8, 1024), F32),
            vm((4, 8, 1024), F32),
            vm((32, 1024), F32),
            vm((128, 1024), BF16),
            vm((16, 128 * ngy), F32),
            vm((256, 128 * ngy), BF16),
            vm((96, 128 * ngy), BF16),
            vm((2, 8, 1024), F32),
            vm((2, 8, 128), F32),
            vm((4, 8, 128), F32),
            vm((32, 128), F32),
            vm((ngy, 128), F32),
            vm((2, ngy, 128), F32),
            vm((128, 128), F32),
            vm((128, 128), F32),
            vm((96, 256), F32),
            vm((48, 256), F32),
            vm((32, 128), F32),
            vm((8, 128), F32),
            vm((4, 8, 128), F32),
            vm((8, 128), F32),
            vm((ngy // 4, 8, 128), F32),
            vm((8, 128), F32),
            vm((ngx, 8, 128), F32),
            vm((1, 128), F32),
            vm((ngy, 128), F32),
            vm((1, 128), F32),
            vm((ngx, 128), F32),
            dma((24,)),
            dma((8,)),
            dma((8,)),
            dma((8,)),
            dma((8,)),
            dma((7,)),
            dma((7,)),
            dma((2,)),
            dma((2,)),
            pltpu.SemaphoreType.REGULAR((2,)),
        ],
        compiler_params=pltpu.CompilerParams(
            collective_id=0, has_side_effects=True, vmem_limit_bytes=48 * 1024 * 1024
        ),
    )(
        in_hbm(pressure), in_hbm(divergence), in_hbm(diagonal), in_hbm(normals), in_hbm(traction), in_hbm(slot_of),
        in_hbm(slot_of.reshape(8 * ngy, 128)), in_hbm(previous), in_hbm(v), in_hbm(w),
    )
    return pl.pallas_call(
        finish,
        out_shape=(
            jax.ShapeDtypeStruct(pressure.shape, F32),
            jax.ShapeDtypeStruct(previous.shape, F32),
        ),
        in_specs=[vmem] * 7,
        out_specs=(hbm, hbm),
        scratch_shapes=[vm((3, 3072), F32), dma((2,))],
        compiler_params=pltpu.CompilerParams(vmem_limit_bytes=4 * 1024 * 1024),
    )(p_new, *rest)


def solution(mesh):
    placed = (
        P("gx", "gy", None),
        P("gx", "gy", None),
        P("gx", "gy", None),
        P(None, ("gx", "gy")),
        P(None, ("gx", "gy")),
        P("gx", None),
        P(("gx", "gy")),
        P(None, ("gx", "gy")),
        P(None, None, ("gx", "gy")),
        P(None, None, ("gx", "gy")),
    )
    return jax.shard_map(
        functools.partial(shards, mesh.shape["gx"], mesh.shape["gy"]),
        mesh=mesh,
        in_specs=placed,
        out_specs=(P("gx", "gy", None), P(None, ("gx", "gy"))),
        check_vma=False,
    )
```
